256 devices in a mesh: gx: 8 (over x, core), gy: 8 (over z), gz: 4 (over y).
Axes of the slice: x: 4, y: 4, z: 8, core: 2. Of those that a mesh axis runs over, the one named last changes fastest.
Arguments:
- pair_list: int32 [8192, 2], P(('gx', 'gy', 'gz')), may hold values from 0 to 63, all different within a row; in each aligned block of 32 rows (0 to 31, 32 to 63, ...) at most 2 rows name the same one
- rank_bucket: int32 [8192], P(('gx', 'gy', 'gz')), may hold values from 0 to 2
- amplitudes: bfloat16 [8192, 36864], P(('gx', 'gy', 'gz')), may hold values from -0.4375 to 0.4375
- intersects: bfloat16 [8192, 36864], P(('gx', 'gy', 'gz')), may hold values from -0.4375 to 0.4375
- integrals: bfloat16 [8192, 36864], P(('gx', 'gy', 'gz')), may hold values from -6 to 6
- exchange_blocks: bfloat16 [64, 36864], P(('gx', 'gy')), may hold values from -0.4375 to 0.4375
Outputs:
- residuals: bfloat16 [8192, 36864], P(('gx', 'gy', 'gz'))
The draws below stay inside these ranges and needn't reach their ends.
Inputs may be any that keep to these rules, and one draw needn't show every extreme that they name: `pair_list`: each row names two different occupied orbitals; within the rows of one device no orbital is named more than 2 times, a bound that some block reaches on some devices. `rank_bucket`: bucket b keeps the leading (b + 1) * 64 PNOs.
All inputs are finite; a program needn't handle non-finite values.
Results may differ from the reference program's by a relative error of at most 0.013.
Values may be sent and summed in bfloat16 or wider, within the bound.
A program may use at most 128 MiB of HBM per device.

```python
import math
import jax
import jax.numpy as jnp
import numpy as np
from jax import lax

RSTEP = 64
R = 192
NOCC = 64
MOST = 2
PAIR_DEV = 32
NPAIRS = 8192


def touch_ends(values, stream_key, least, top_value):
    place = [jax.random.randint(jax.random.fold_in(stream_key, axis), (), 0, length) for axis, length in enumerate(values.shape)]
    main_axis = values.shape.index(max(values.shape))
    neighbour = place[:main_axis] + [(place[main_axis] + 1) % values.shape[main_axis]] + place[main_axis + 1:]
    return values.at[tuple(place)].set(least).at[tuple(neighbour)].set(top_value)


def levels(key, shape, split, least, high):
    def one(dim, parts):
        heights = jax.random.uniform(jax.random.fold_in(jax.random.fold_in(key, 6), dim), (parts,), jnp.float32, least / len(split), high / len(split))
        return jnp.repeat(jnp.exp(heights), shape[dim] // parts).reshape((-1,) + (1,) * (len(shape) - dim - 1))

    gain = one(*split[0])
    for cut in split[1:]:
        gain = gain * one(*cut)
    return gain


def deal_out(rng, own, number, rows, amount, top, bound, lean):
    order = jax.random.permutation(rng, amount)
    heavy_load, ordinary = load_shares(amount, rows * top, bound, lean, True), load_shares(amount, rows * top, bound, lean, False)
    places = jnp.arange(amount)

    def named(tallies, turn):
        used = int((tallies > 0).sum())
        fixed = max(1, used // 4)
        passed = fixed + (places - fixed + turn * (used - fixed)) % max(1, amount - fixed)
        return jnp.zeros((amount,), jnp.int32).at[order[jnp.where(places < fixed, places, passed)]].set(jnp.asarray(tallies, jnp.int32))

    tallies = jnp.where(number % 4 == 0, named(heavy_load, number // 4), named(ordinary, number - number // 4 - 1))
    mixed = jax.random.permutation(jax.random.fold_in(own, 3), amount)
    giver, receiver = mixed[0:amount // 2 * 2:2], mixed[1:amount // 2 * 2:2]
    slack = jnp.minimum(tallies[giver] - 1, bound - tallies[receiver]) // 2
    slack = jnp.where((giver == order[0]) | (receiver == order[0]) | (tallies[receiver] == 0), 0, jnp.maximum(slack, 0))
    passed = jax.random.randint(jax.random.fold_in(own, 4), (amount // 2,), 0, 1 << 20) % (slack + 1)
    tallies = tallies.at[giver].add(-passed).at[receiver].add(passed)
    items = jnp.searchsorted(jnp.cumsum(tallies), jnp.arange(rows * top), side="right").astype(jnp.int32)
    listing = items.reshape(top, rows).T
    listing = listing[jax.random.permutation(jax.random.fold_in(own, 1), rows)]
    turn = jax.random.randint(jax.random.fold_in(own, 2), (rows, 1), 0, top)
    return jnp.take_along_axis(listing, (jnp.arange(top)[None, :] + turn) % top, axis=1)


def load_shares(count, total, bound, slope, full):
    portions = [(1 << 20) // math.isqrt(standing ** slope) + 1 for standing in range(1, count + 1)]
    largest = bound if full else min(bound, max(-(-total // count), total * portions[0] // sum(portions)))
    least = 1 if total - largest >= count - 1 else 0
    holding, surplus = [largest] + [least] * (count - 1), total - largest - least * (count - 1)
    while surplus > 0:
        movable = [i for i in range(1, count) if holding[i] < largest] or [i for i in range(1, count) if holding[i] < bound]
        pool, remaining = sum([portions[i] for i in movable]), surplus
        for i in movable:
            extra = min(bound - holding[i], max(1, remaining * portions[i] // pool), surplus)
            holding[i] = holding[i] + extra
            surplus = surplus - extra
    return np.array(holding)


def scatter_about(rng, shape, scale, limit, cuts=(), kind=jnp.bfloat16):
    values = scale * jax.random.normal(rng, shape, jnp.float32)
    if cuts:
        values = values * levels(rng, shape, cuts, -0.22, 0.18)
    return jnp.clip(values, -limit, limit).astype(kind)


def setup_inputs(seed: int = 0) -> dict:
    keys = jax.random.split(jax.random.key(seed), 7)
    pair_list_keys = jax.random.split(jax.random.fold_in(keys[0], 1), NPAIRS // PAIR_DEV)
    pair_list_turns = jax.random.permutation(jax.random.fold_in(keys[0], 3), NPAIRS // PAIR_DEV)
    pair_list = jax.vmap(lambda own, number: deal_out(jax.random.fold_in(keys[0], 2), own, number, PAIR_DEV, NOCC, 2, MOST, 2))(pair_list_keys, pair_list_turns).reshape((NPAIRS, 2))
    rank_bucket = touch_ends(jax.random.randint(keys[1], (NPAIRS,), 0, 3), jax.random.fold_in(keys[1], 1), 0, 2).astype(jnp.int32)
    amplitudes = scatter_about(keys[2], (NPAIRS, R * R), R ** -0.5, 0.4375, ((0, 256),))
    intersects = scatter_about(keys[3], (NPAIRS, R * R), R ** -0.5, 0.4375, ((0, 256),))
    integrals = scatter_about(keys[4], (NPAIRS, R * R), 1.0, 6.0, ((0, 256),))
    exchange_blocks = scatter_about(keys[5], (NOCC, R * R), R ** -0.5, 0.4375, ((0, 64),))
    return {"pair_list": pair_list, "rank_bucket": rank_bucket, "amplitudes": amplitudes, "intersects": intersects, "integrals": integrals, "exchange_blocks": exchange_blocks}


def rounded(value):
    return lax.optimization_barrier(value.astype(jnp.bfloat16)).astype(jnp.float32)


def rank_mask(bucket):
    rank_size = (bucket + 1) * RSTEP
    row_index = jnp.arange(R, dtype=jnp.int32)
    return (row_index[None, :, None] < rank_size[:, None, None]) & (row_index[None, None, :] < rank_size[:, None, None])


def project_block(inputs):
    bucket, amplitude, intersect = inputs
    inside = rank_mask(bucket)
    masked = jnp.where(inside, amplitude, jnp.zeros_like(amplitude))
    half_projected = rounded(jnp.einsum('pab,pbc->pac', intersect.astype(jnp.float32), masked.astype(jnp.float32)))
    return jnp.einsum('pab,pcb->pac', half_projected, intersect.astype(jnp.float32)).astype(jnp.bfloat16)


def reference(pair_list, rank_bucket, amplitudes, intersects, integrals, exchange_blocks):
    blocks = NPAIRS // PAIR_DEV
    block_shape = (blocks, PAIR_DEV, R, R)
    exchange_square = exchange_blocks.reshape(NOCC, R, R)
    bucket_blocks = rank_bucket.reshape(blocks, PAIR_DEV)
    list_blocks = pair_list.reshape(blocks, PAIR_DEV, 2)
    amplitude_blocks = amplitudes.reshape(block_shape)
    intersect_blocks = intersects.reshape(block_shape)
    integral_blocks = integrals.reshape(block_shape)
    projected = lax.map(project_block, (bucket_blocks, amplitude_blocks, intersect_blocks))

    def accumulate(domain, inputs):
        ends_block, projected_block = inputs
        as_float = projected_block.astype(jnp.float32)
        domain = domain + jax.ops.segment_sum(as_float, ends_block[:, 0], num_segments=NOCC)
        domain = domain + jax.ops.segment_sum(as_float, ends_block[:, 1], num_segments=NOCC)
        return domain, None

    domain, unused = lax.scan(accumulate, jnp.zeros((NOCC, R, R), jnp.float32), (list_blocks, projected))
    coupled = rounded(jnp.einsum('oab,obc->oac', rounded(domain), exchange_square.astype(jnp.float32)))

    def finish(inputs):
        ends_block, bucket, projected_block, intersect, integral, amplitude = inputs
        inside = rank_mask(bucket)
        masked = jnp.where(inside, amplitude, jnp.zeros_like(amplitude))
        combined = jnp.zeros((PAIR_DEV, R, R), jnp.float32)
        for which_end in range(2):
            orbital = ends_block[:, which_end]
            own_term = rounded(jnp.einsum('pab,pbc->pac', projected_block.astype(jnp.float32), exchange_square[orbital].astype(jnp.float32)))
            answer = rounded(coupled[orbital] - own_term)
            combined = combined + answer
        combined = rounded(combined)
        half_back = rounded(jnp.einsum('pba,pbc->pac', intersect.astype(jnp.float32), combined))
        back_projected = jnp.einsum('pab,pbc->pac', half_back, intersect.astype(jnp.float32))
        local_term = jnp.einsum('pab,pbc->pac', masked.astype(jnp.float32), integral.astype(jnp.float32))
        residual_sum = integral.astype(jnp.float32) + local_term + back_projected
        return jnp.where(inside, residual_sum, jnp.zeros_like(residual_sum)).astype(jnp.bfloat16)

    result = lax.map(finish, (list_blocks, bucket_blocks, projected, intersect_blocks, integral_blocks, amplitude_blocks))
    return result.reshape(NPAIRS, R * R)
```

```python
import functools

import jax
import jax.numpy as jnp
from jax import lax
from jax.experimental import pallas as pl
from jax.experimental.pallas import tpu as pltpu
from jax.sharding import Mesh
from jax.sharding import PartitionSpec as P

RSTEP = 64
R = 192
Q = 48
CH = 80
GX_GY = ("gx_0", "gx_1", "gy")
GX_GY_GZ = ("gx_0", "gx_1", "gy", "gz")
MESH = pl.DeviceIdType.MESH
BF = jnp.bfloat16
F32 = jnp.float32


def pack(v):
    right = jnp.concatenate([v[:, 128:192], jnp.zeros((Q, 64), F32)], axis=1)
    first = right[0:16] + pltpu.roll(right[16:32], 64, 1)
    return jnp.concatenate([v[:, 0:128], first, right[32:48]], axis=0)


def unpack(c):
    first = c[48:64]
    right = jnp.concatenate([first, pltpu.roll(first, 64, 1), c[64:80]], axis=0)
    return jnp.concatenate([c[0:48], right], axis=1)


def dot(a, b, ca, cb):
    return lax.dot_general(a, b, (((ca,), (cb,)), ((), ())), preferred_element_type=F32)


def masked_block(t, rank):
    row = lax.broadcasted_iota(jnp.int32, (R, R), 0)
    col = lax.broadcasted_iota(jnp.int32, (R, R), 1)
    inside = (row < rank) & (col < rank)
    return inside, jnp.where(inside, t.astype(F32), 0.0)


def project_kernel(pairs, ranks, s_ref, t_ref, p_ref, dom_ref):
    p = pl.program_id(0)

    @pl.when(p == 0)
    def _():
        @pl.loop(0, 16)
        def _(i):
            dom_ref[i] = jnp.zeros(dom_ref.shape[1:], BF)

    s = s_ref[0]
    _, m = masked_block(t_ref[0], (ranks[p] + 1) * RSTEP)
    half = dot(s, m.astype(BF), 1, 0).astype(BF)
    full = dot(half, s, 1, 1).astype(BF)
    p_ref[0] = full
    full = full.astype(F32)
    for q in range(4):
        quarter = pack(full[Q * q : Q * q + Q])
        for e in range(2):
            k = pairs[2 * p + e]
            at = dom_ref.at[k // 4, q, k % 4]
            at[...] = (at[...].astype(F32) + quarter).astype(BF)


def exchange_kernel(dom, x_ref, gc, gx, rc_a, rc_b, acc_a, acc_b, tr_a, rx_a, tr_b, rx_b, tr_c, rx_c, tr_d, rx_d, zb, zr, send_sem, recv_sem):
    x, c, z, y = (lax.axis_index(a) for a in GX_GY_GZ)
    barrier = pltpu.get_barrier_semaphore()
    peers = [{"gx_1": 1 - c}]
    peers += [{"gx_0": (x + d) % 4} for d in (1, 3)]
    peers += [{"gz": (y + d) % 4} for d in (1, 3)]
    peers += [{"gy": (z + d) % 8} for d in range(1, 8)]
    for who in peers:
        pl.semaphore_signal(barrier, inc=1, device_id=who, device_id_type=MESH)
    pl.semaphore_wait(barrier, len(peers))

    started = []

    def send(src, dst, who):
        i = len(started)
        copy = pltpu.make_async_remote_copy(
            src_ref=src, dst_ref=dst, send_sem=send_sem.at[i], recv_sem=recv_sem.at[i], device_id=who, device_id_type=MESH
        )
        copy.start()
        started.append(copy)
        return copy

    def core(src, dst):
        return send(src, dst, {"gx_1": 1 - c})

    def add2(dst, i, a, b):
        dst[...] = (a[...].astype(F32) + b[...].astype(F32)).astype(BF)

    def add_into(n1, n2, dst, src):
        @pl.loop(0, n1)
        def _(i):
            for j in range(n2):
                dst[i, j] = (dst[i, j].astype(F32) + src[i, j].astype(F32)).astype(BF)

    def gather(g):
        g7 = g.reshape(4, 2, 2, 4, 4, CH, 128)

        over = []

        def across(ref):
            over.append(core(ref, ref))

        def at_own():
            return g.at[(x * 2 + c) * 2 + z // 4, y, z % 4]

        zc = [send(at_own(), at_own(), {"gy": (z + d) % 8}) for d in range(1, 8)]
        yield
        for copy in zc:
            copy.wait_recv()

        def piece_a2(q):
            return g.at[(x * 2 + c) * 2, q]

        def piece_b2(xx):
            return g.at[(xx * 2 + c) * 2 + 1, y]

        def piece_a3(xx):
            return g.at[(xx * 2 + c) * 2]

        def piece_b3(q):
            return g7.at[:, c, 1, q]

        def rings(specs, forward):
            copies = []
            for axis, pos, piece, half, n in specs:
                own = piece(pos)
                up = send(own, own, {axis: (pos + 1) % 4})
                down = send(own, own, {axis: (pos + 3) % 4})
                copies.append((up, down))
            if forward:
                for axis, pos, piece, half, n in specs:
                    across(piece(pos))
            yield
            second = []
            for (axis, pos, piece, half, n), (up, down) in zip(specs, copies):
                up.wait_recv()
                got = piece((pos + 3) % 4)
                low = send(got.at[0:half], got.at[0:half], {axis: (pos + 1) % 4})
                if forward:
                    across(got)
                down.wait_recv()
                got = piece((pos + 1) % 4)
                high = send(got.at[half:n], got.at[half:n], {axis: (pos + 3) % 4})
                if forward:
                    across(got)
                second.append((low, high))
            yield
            for (axis, pos, piece, half, n), (low, high) in zip(specs, second):
                got = piece((pos + 2) % 4)
                low.wait_recv()
                if forward:
                    across(got.at[0:half])
                high.wait_recv()
                if forward:
                    across(got.at[half:n])

        yield from rings([("gz", y, piece_a2, 2, 4), ("gx_0", x, piece_b2, 2, 4)], False)
        yield from rings([("gx_0", x, piece_a3, 2, 4), ("gz", y, piece_b3, 2, 4)], True)
        yield
        for copy in over:
            copy.wait_recv()

    own = pack(x_ref[pl.ds(pl.multiple_of(Q * y, Q), Q), :].astype(F32)).astype(BF)
    gx[(x * 2 + c) * 2 + z // 4, y, z % 4] = own

    dom7 = dom.reshape(4, 2, 2, 4, 4, CH, 128)
    order = (2, 1, 3, 0)
    first = []
    for d in order:
        xx, q = (x + d) % 4, (y + d) % 4
        first.append(
            (
                xx,
                q,
                core(dom7.at[xx, 1 - c, 0], rc_a.at[xx]),
                core(dom7.at[:, 1 - c, 1, q], rc_b.at[q]),
            )
        )

    gather_x = gather(gx)
    next(gather_x)

    def ring_reduce(specs):
        state = []
        for axis, pos, acc, n, transit, arrived, ready in specs:
            h = n // 2
            up, down = {axis: (pos + 1) % 4}, {axis: (pos + 3) % 4}
            pu, pd, far = (pos + 1) % 4, (pos + 3) % 4, (pos + 2) % 4
            ready(2)
            t_up = send(acc.at[far, 0:h], transit.at[0], up)
            t_dn = send(acc.at[far, h:n], transit.at[1], down)
            state.append([up, down, pu, pd, t_up, t_dn])
        for (axis, pos, acc, n, transit, arrived, ready), st in zip(specs, state):
            h = n // 2
            up, down, pu, pd, t_up, t_dn = st
            ready(1)
            a = send(acc.at[pu, h:n], arrived.at[0, h:n], up)
            ready(3)
            b = send(acc.at[pd, 0:h], arrived.at[1, 0:h], down)
            st += [a, b]
        for (axis, pos, acc, n, transit, arrived, ready), st in zip(specs, state):
            ready(0)
        yield
        for (axis, pos, acc, n, transit, arrived, ready), st in zip(specs, state):
            h = n // 2
            up, down, pu, pd, t_up, t_dn, a, b = st
            t_up.wait_recv()
            add_half(acc.at[pu, 0:h], transit.at[0])
            e = send(acc.at[pu, 0:h], arrived.at[0, 0:h], up)
            t_dn.wait_recv()
            add_half(acc.at[pd, h:n], transit.at[1])
            f = send(acc.at[pd, h:n], arrived.at[1, h:n], down)
            st += [e, f]
        yield
        for (axis, pos, acc, n, transit, arrived, ready), st in zip(specs, state):
            for copy in st[6:10]:
                copy.wait_recv()

    def add_half(dst, src):
        if len(dst.shape) == 4:
            add_into(dst.shape[0], dst.shape[1], dst, src)
        else:
            for j in range(dst.shape[0]):
                dst[j] = (dst[j].astype(F32) + src[j].astype(F32)).astype(BF)

    def ready_a(d):
        xx, q, ca, cb = first[order.index(d)]
        ca.wait_recv()

        @pl.loop(0, 4)
        def _(i):
            for j in range(4):
                acc_a[xx, i, j] = (dom[(xx * 2 + c) * 2, i, j].astype(F32) + rc_a[xx, i, j].astype(F32)).astype(BF)

    def ready_b(d):
        xx, q, ca, cb = first[order.index(d)]
        cb.wait_recv()

        @pl.loop(0, 4)
        def _(i):
            for j in range(4):
                acc_b[q, i, j] = (dom[(i * 2 + c) * 2 + 1, q, j].astype(F32) + rc_b[q, i, j].astype(F32)).astype(BF)

    ring = ring_reduce(
        [("gx_0", x, acc_a, 4, tr_a, rx_a, ready_a), ("gz", y, acc_b, 4, tr_b, rx_b, ready_b)]
    )
    next(ring)
    next(gather_x)
    next(ring)
    next(gather_x)
    for _ in ring:
        pass

    @pl.loop(0, 4)
    def _(i):
        for j in range(4):
            for acc, pos, arrived in ((acc_a, x, rx_a), (acc_b, y, rx_b)):
                acc[pos, i, j] = (acc[pos, i, j].astype(F32) + arrived[0, i, j].astype(F32) + arrived[1, i, j].astype(F32)).astype(BF)

    def nothing(d):
        return None

    ring = ring_reduce(
        [("gz", y, acc_a.at[x], 4, tr_c, rx_c, nothing), ("gx_0", x, acc_b.at[y], 4, tr_d, rx_d, nothing)]
    )
    next(ring)
    next(gather_x)
    next(ring)
    for _ in ring:
        pass
    for j in range(4):
        zb[j] = (acc_a[x, y, j].astype(F32) + rx_c[0, j].astype(F32) + rx_c[1, j].astype(F32)).astype(BF)
        zb[4 + j] = (acc_b[y, x, j].astype(F32) + rx_d[0, j].astype(F32) + rx_d[1, j].astype(F32)).astype(BF)

    zc = [send(zb.at[(z + d) % 8], zr.at[d - 1], {"gy": (z + d) % 8}) for d in range(1, 8)]
    next(gather_x)
    for copy in zc:
        copy.wait_recv()
    total = zb[z].astype(F32)
    for d in range(7):
        total = total + zr[d].astype(F32)
    domain = unpack(total)[:, 0:R].astype(BF)
    coupled = dot(domain, x_ref[...], 1, 0)
    gc[(x * 2 + c) * 2 + z // 4, y, z % 4] = pack(coupled).astype(BF)

    for _ in gather(gc):
        pass
    for _ in gather_x:
        pass
    for copy in started:
        copy.wait_send()


def finish_kernel(pairs, ranks, s_ref, t_ref, v_ref, p_ref, gc, gx, o_ref):
    p = pl.program_id(0)
    k0, k1 = pairs[2 * p], pairs[2 * p + 1]

    def both(g):
        parts = [
            unpack(g[k0 // 4, q, k0 % 4].astype(F32) + g[k1 // 4, q, k1 % 4].astype(F32)) for q in range(4)
        ]
        return jnp.concatenate(parts, axis=0)

    inside, m = masked_block(t_ref[0], (ranks[p] + 1) * RSTEP)
    s, v = s_ref[0], v_ref[0]
    own = dot(p_ref[0], both(gx).astype(BF), 1, 0)
    combined = (both(gc) - own)[:, 0:R].astype(BF)
    half = dot(combined, s, 1, 0).astype(BF)
    back = dot(s, half, 0, 0)
    local = dot(m.astype(BF), v, 1, 0)
    o_ref[0] = jnp.where(inside, v.astype(F32) + local + back, 0.0).astype(BF)


def body(pair_list, rank_bucket, amplitudes, intersects, integrals, exchange_blocks):
    n = amplitudes.shape[0]
    t = amplitudes.reshape(n, R, R)
    s = intersects.reshape(n, R, R)
    v = integrals.reshape(n, R, R)
    xb = exchange_blocks.reshape(R, R)
    pairs = pair_list.reshape(2 * n)
    block = pl.BlockSpec((1, R, R), lambda p, *_: (p, 0, 0))
    gathered = (16, 4, 4, CH, 128)
    whole = pl.BlockSpec(gathered, lambda p, *_: (0, 0, 0, 0, 0))
    projected, dom = pl.pallas_call(
        project_kernel,
        grid_spec=pltpu.PrefetchScalarGridSpec(
            num_scalar_prefetch=2, grid=(n,), in_specs=[block, block], out_specs=[block, whole]
        ),
        out_shape=[jax.ShapeDtypeStruct((n, R, R), BF), jax.ShapeDtypeStruct(gathered, BF)],
        compiler_params=pltpu.CompilerParams(vmem_limit_bytes=40 * 2**20),
    )(pairs, rank_bucket, s, t)

    vm = pl.BlockSpec(memory_space=pltpu.VMEM)
    tail = (CH, 128)
    gc, gx = pl.pallas_call(
        exchange_kernel,
        in_specs=[vm, vm],
        out_specs=[vm, vm],
        out_shape=[jax.ShapeDtypeStruct(gathered, BF)] * 2,
        scratch_shapes=[
            pltpu.VMEM((4, 4, 4) + tail, BF),
            pltpu.VMEM((4, 4, 4) + tail, BF),
            pltpu.VMEM((4, 4, 4) + tail, BF),
            pltpu.VMEM((4, 4, 4) + tail, BF),
            pltpu.VMEM((2, 2, 4) + tail, BF),
            pltpu.VMEM((2, 4, 4) + tail, BF),
            pltpu.VMEM((2, 2, 4) + tail, BF),
            pltpu.VMEM((2, 4, 4) + tail, BF),
            pltpu.VMEM((2, 2) + tail, BF),
            pltpu.VMEM((2, 4) + tail, BF),
            pltpu.VMEM((2, 2) + tail, BF),
            pltpu.VMEM((2, 4) + tail, BF),
            pltpu.VMEM((8,) + tail, BF),
            pltpu.VMEM((7,) + tail, BF),
            pltpu.SemaphoreType.DMA((128,)),
            pltpu.SemaphoreType.DMA((128,)),
        ],
        compiler_params=pltpu.CompilerParams(collective_id=0, has_side_effects=True, vmem_limit_bytes=60 * 2**20),
    )(dom, xb)

    out = pl.pallas_call(
        finish_kernel,
        grid_spec=pltpu.PrefetchScalarGridSpec(
            num_scalar_prefetch=2,
            grid=(n,),
            in_specs=[block, block, block, block, whole, whole],
            out_specs=block,
        ),
        out_shape=jax.ShapeDtypeStruct((n, R, R), BF),
        compiler_params=pltpu.CompilerParams(vmem_limit_bytes=40 * 2**20),
    )(pairs, rank_bucket, s, t, v, projected, gc, gx)
    return out.reshape(n, R * R)


def solution(mesh):
    torus = Mesh(mesh.devices.reshape(4, 2, mesh.shape["gy"], mesh.shape["gz"]), GX_GY_GZ)
    return jax.shard_map(
        body,
        mesh=torus,
        in_specs=(
            P(GX_GY_GZ, None),
            P(GX_GY_GZ),
            P(GX_GY_GZ, None),
            P(GX_GY_GZ, None),
            P(GX_GY_GZ, None),
            P(GX_GY, None),
        ),
        out_specs=P(GX_GY_GZ, None),
        check_vma=False,
    )
```

```python
import jax
import jax.numpy as jnp
from jax import lax
from jax.experimental import pallas as pl
from jax.experimental.pallas import tpu as pltpu
from jax.sharding import Mesh
from jax.sharding import PartitionSpec as P

RSTEP = 64
R = 192
W = 256
Q = 48
CH = 72
LINES = R * R // 128
GX_GY = ("gx_0", "gx_1", "gy")
GX_GY_GZ = ("gx_0", "gx_1", "gy", "gz")
MESH = pl.DeviceIdType.MESH
BF = jnp.bfloat16
F32 = jnp.float32


def pack(v):
    right = v[:, 128:256]
    return jnp.concatenate([v[:, 0:128], right[0:24] + pltpu.roll(right[24:48], 64, 1)], axis=0)


def unpack(c):
    right = jnp.concatenate([c[48:72], pltpu.roll(c[48:72], 64, 1)], axis=0)
    return jnp.concatenate([c[0:48], right], axis=1)


def dot(a, b, ca=1, cb=0):
    return lax.dot_general(a, b, (((ca,), (cb,)), ((), ())), preferred_element_type=F32)


def low_lanes(n):
    return lax.broadcasted_iota(jnp.int32, (n, 128), 1) < 64


def even_odd(l0, l1, l2):
    low = low_lanes(l0.shape[0])
    t1, t2 = pltpu.roll(l1, 64, 1), pltpu.roll(l2, 64, 1)
    return (l0, jnp.where(low, l1, 0.0)), (jnp.where(low, t1, t2), jnp.where(low, t2, 0.0))


def kernel(
    inv, ranks, t_hbm, s_hbm, v_hbm, x_raw, o_hbm,
    s_raw, t_raw, v_raw, lines, xl, tmp, s_sq, m_sq, v_sq, x_sq, w_sq, st, pq, base, pp,
    gc, gx, sb_a, sb_b, rc_a, rc_b, acc_a, acc_b, tr_a, rx_a, tr_b, rx_b, tr_c, rx_c, tr_d, rx_d, zb, zr,
    pairs, load_sem, store_sem, send_sem, recv_sem,
):
    n = s_raw.shape[0]
    x, c, z, y = (lax.axis_index(a) for a in GX_GY_GZ)
    loads = []
    for i, (src, dst) in enumerate(((s_hbm, s_raw), (t_hbm, t_raw), (v_hbm, v_raw))):
        for g in range(n // 8):
            copy = pltpu.make_async_copy(src.at[8 * g : 8 * g + 8], dst.at[8 * g : 8 * g + 8], load_sem.at[i, g])
            copy.start()
            loads.append(copy)

    barrier = pltpu.get_barrier_semaphore()
    peers = [{"gx_1": 1 - c}]
    peers += [{"gx_0": (x + d) % 4} for d in (1, 3)]
    peers += [{"gz": (y + d) % 4} for d in (1, 3)]
    peers += [{"gy": (z + d) % 8} for d in range(1, 8)]
    for who in peers:
        pl.semaphore_signal(barrier, inc=1, device_id=who, device_id_type=MESH)

    started = []

    def send(src, dst, who):
        i = len(started)
        copy = pltpu.make_async_remote_copy(
            src_ref=src, dst_ref=dst, send_sem=send_sem.at[i], recv_sem=recv_sem.at[i], device_id=who, device_id_type=MESH
        )
        copy.start()
        started.append(copy)
        return copy

    def core(src, dst):
        return send(src, dst, {"gx_1": 1 - c})

    def gather(g):
        over = []

        def across(ref):
            over.append(core(ref, ref))

        own = g.at[x, c, z // 4, y, z % 4]
        zc = [send(own, own, {"gy": (z + d) % 8}) for d in range(1, 8)]
        yield
        for copy in zc:
            copy.wait_recv()

        def piece_a2(q):
            return g.at[x, c, 0, q]

        def piece_b2(xx):
            return g.at[xx, c, 1, y]

        def piece_a3(xx):
            return g.at[xx, c, 0]

        def piece_b3(q):
            return g.at[:, c, 1, q]

        def rings(specs, forward):
            copies = []
            for axis, pos, piece, half in specs:
                own = piece(pos)
                up = send(own, own, {axis: (pos + 1) % 4})
                down = send(own, own, {axis: (pos + 3) % 4})
                copies.append((up, down))
            if forward:
                for axis, pos, piece, half in specs:
                    across(piece(pos))
            yield
            second = []
            for (axis, pos, piece, half), (up, down) in zip(specs, copies):
                up.wait_recv()
                got = piece((pos + 3) % 4)
                low = send(got.at[0:half], got.at[0:half], {axis: (pos + 1) % 4})
                if forward:
                    across(got)
                down.wait_recv()
                got = piece((pos + 1) % 4)
                high = send(got.at[half:4], got.at[half:4], {axis: (pos + 3) % 4})
                if forward:
                    across(got)
                second.append((low, high))
            yield
            for (axis, pos, piece, half), (low, high) in zip(specs, second):
                got = piece((pos + 2) % 4)
                low.wait_recv()
                if forward:
                    across(got.at[0:half])
                high.wait_recv()
                if forward:
                    across(got.at[half:4])

        yield from rings([("gz", y, piece_a2, 2), ("gx_0", x, piece_b2, 2)], False)
        yield from rings([("gx_0", x, piece_a3, 2), ("gz", y, piece_b3, 2)], True)
        yield
        for copy in over:
            copy.wait_recv()

    @pl.loop(0, LINES // 8)
    def _(i):
        for u in range(8):
            xl[pl.ds(i * 8 + u, 1), :] = x_raw[0:1, pl.ds(pl.multiple_of((i * 8 + u) * 128, 128), 128)].astype(F32)

    even, odd = even_odd(*(xl[pl.ds(i, 96, stride=3), :] for i in range(3)))
    at = lax.broadcasted_iota(jnp.int32, (W, W), 1)
    to = jnp.where(at < 96, 2 * at, jnp.where(at < R, 2 * at - (R - 1), -1))
    turn = (lax.broadcasted_iota(jnp.int32, (W, W), 0) == to).astype(F32).astype(BF)
    for i, half in enumerate((even, odd)):
        x_sq[96 * i : 96 * i + 96, :] = dot(jnp.concatenate(half, axis=1).astype(BF), turn).astype(BF)
    x_sq[R:W, :] = jnp.zeros((W - R, W), BF)
    gx[x, c, z // 4, y, z % 4] = pack(
        x_sq[pl.ds(pl.multiple_of(Q * y, Q), Q), :].astype(F32)
    ).astype(BF)
    for i in range(2):
        w_sq[i, R:W, :] = jnp.zeros((W - R, W), BF)
        v_sq[i, R:W, :] = jnp.zeros((W - R, W), BF)
    pp[n] = jnp.zeros((4, CH, 128), BF)

    pl.semaphore_wait(barrier, len(peers))
    gather_x = gather(gx)
    next(gather_x)

    def to_lines(raw, g):
        @pl.loop(0, LINES // 12)
        def _(i):
            for u in range(12):
                at = i * 12 + u
                lines[pl.ds(pl.multiple_of(at * 8, 8), 8), :] = raw[
                    8 * g : 8 * g + 8, pl.ds(pl.multiple_of(at * 128, 128), 128)
                ].astype(F32)

    def halves(p):
        return even_odd(*(lines[pl.ds(8 * i + p, 96, stride=24), :] for i in range(3)))

    def natural(p, u):
        for i, half in enumerate(halves(p)):
            for j in range(2):
                tmp[u, j, pl.ds(i, 96, stride=2), :] = half[j]
        return square(u)

    def square(u):
        return jnp.concatenate([tmp[u, 0], tmp[u, 1]], axis=1)

    row = lax.broadcasted_iota(jnp.int32, (R, W), 0)
    col = lax.broadcasted_iota(jnp.int32, (R, W), 1)
    far = jnp.maximum(row, col)

    def project(g):
        loads[g].wait()
        to_lines(s_raw, g)

        @pl.loop(0, 8)
        def _(p):
            at = 8 * g + p
            for i, half in enumerate(halves(p)):
                s_sq[at, 96 * i : 96 * i + 96, :] = jnp.concatenate(half, axis=1).astype(BF)
            s_sq[at, R:W, :] = jnp.zeros((W - R, W), BF)

        loads[n // 8 + g].wait()
        to_lines(t_raw, g)

        @pl.loop(0, 4)
        def _(i):
            for u in range(2):
                p = 2 * i + u
                at = 8 * g + p
                m_sq[at, 0:R, :] = jnp.where(far < (ranks[at] + 1) * RSTEP, natural(p, u), 0.0).astype(BF)
                m_sq[at, R:W, :] = jnp.zeros((W - R, W), BF)
            for u in range(2):
                at = 8 * g + 2 * i + u
                half = dot(s_sq[at, 0:R, :], m_sq[at]).astype(BF)
                full = dot(half, s_sq[at], 1, 1).astype(BF)
                pq[at] = full
                full = full.astype(F32)
                for q in range(4):
                    pp[at, q] = pack(full[Q * q : Q * q + Q]).astype(BF)

    for g in range(n // 8):
        project(g)
        if g < 3:
            next(gather_x)

    def transposes(g):
        @pl.loop(0, 8)
        def _(p):
            st[8 * g + p] = s_sq[8 * g + p].T[0:R]

    def local(g):
        loads[2 * (n // 8) + g].wait()
        to_lines(v_raw, g)

        @pl.loop(0, 4)
        def _(i):
            for u in range(2):
                v_sq[u, 0:R, :] = natural(2 * i + u, u).astype(BF)
            for u in range(2):
                at = 8 * g + 2 * i + u
                base[at] = square(u) + dot(m_sq[at, 0:R, :], v_sq[u])

    def block(g, k, q):
        return g[k // 16, k // 8 % 2, k // 4 % 2, q, k % 4].astype(F32)

    def both(g, at):
        k0, k1 = pairs[2 * at], pairs[2 * at + 1]
        return jnp.concatenate(
            [unpack(block(g, k0, q) + block(g, k1, q)) for q in range(4)], axis=0
        )

    def own_terms(g):
        @pl.loop(0, 4)
        def _(i):
            for u in range(2):
                at = 8 * g + 2 * i + u
                w_sq[u, 0:R, :] = both(gx, at).astype(BF)
            for u in range(2):
                at = 8 * g + 2 * i + u
                pq[at] = dot(pq[at], w_sq[u]).astype(BF)

    early = [lambda g=g: local(g) for g in range(4)] + [lambda g=g: transposes(g) for g in range(4)]
    late = [lambda g=g: own_terms(g) for g in range(4)]

    def fill(work, count):
        for _ in range(count):
            if work:
                work.pop(0)()

    def ends(k):
        return pp[inv[2 * k]].astype(F32) + pp[inv[2 * k + 1]].astype(F32)

    order = (2, 1, 3, 0)
    first_a, first_b = [], []
    for d in order:
        xx = (x + d) % 4

        @pl.loop(0, 4)
        def _(j):
            k = (xx * 2 + 1 - c) * 8 + j
            sb_a[xx, :, j] = ends(k).astype(BF)
            sb_b[:, xx, j] = ends(k + 4).astype(BF)

        first_a.append(core(sb_a.at[xx], rc_a.at[xx]))
    for d in order:
        q = (y + d) % 4
        first_b.append(core(sb_b.at[q], rc_b.at[q]))

    for d in order:
        xx = (x + d) % 4

        @pl.loop(0, 4)
        def _(j):
            k = (xx * 2 + c) * 8 + j
            acc_a[xx, :, j] = ends(k).astype(BF)
            acc_b[:, xx, j] = ends(k + 4).astype(BF)

    def add_into(dst, src):
        if len(dst.shape) == 4:

            @pl.loop(0, dst.shape[0])
            def _(i):
                for j in range(dst.shape[1]):
                    dst[i, j] = (dst[i, j].astype(F32) + src[i, j].astype(F32)).astype(BF)
        else:
            for j in range(dst.shape[0]):
                dst[j] = (dst[j].astype(F32) + src[j].astype(F32)).astype(BF)

    def ready_a(d):
        first_a[order.index(d)].wait_recv()
        add_into(acc_a.at[(x + d) % 4], rc_a.at[(x + d) % 4])

    def ready_b(d):
        first_b[order.index(d)].wait_recv()
        add_into(acc_b.at[(y + d) % 4], rc_b.at[(y + d) % 4])

    def ring_reduce(specs):
        state = []
        for axis, pos, acc, transit, arrived, ready in specs:
            up, down = {axis: (pos + 1) % 4}, {axis: (pos + 3) % 4}
            far = (pos + 2) % 4
            ready(2)
            state.append([up, down, send(acc.at[far, 0:2], transit.at[0], up), send(acc.at[far, 2:4], transit.at[1], down)])
        for (axis, pos, acc, transit, arrived, ready), held in zip(specs, state):
            up, down = held[0:2]
            ready(1)
            held.append(send(acc.at[(pos + 1) % 4, 2:4], arrived.at[0, 2:4], up))
            ready(3)
            held.append(send(acc.at[(pos + 3) % 4, 0:2], arrived.at[1, 0:2], down))
        for spec in specs:
            spec[5](0)
        yield
        for (axis, pos, acc, transit, arrived, ready), held in zip(specs, state):
            up, down, t_up, t_down = held[0:4]
            t_up.wait_recv()
            add_into(acc.at[(pos + 1) % 4, 0:2], transit.at[0])
            held.append(send(acc.at[(pos + 1) % 4, 0:2], arrived.at[0, 0:2], up))
            t_down.wait_recv()
            add_into(acc.at[(pos + 3) % 4, 2:4], transit.at[1])
            held.append(send(acc.at[(pos + 3) % 4, 2:4], arrived.at[1, 2:4], down))
        yield
        for held in state:
            for copy in held[4:8]:
                copy.wait_recv()

    ring = ring_reduce([("gx_0", x, acc_a, tr_a, rx_a, ready_a), ("gz", y, acc_b, tr_b, rx_b, ready_b)])
    next(ring)
    next(gather_x)
    fill(early, 2)
    next(ring)
    next(gather_x)
    fill(early, 3)
    for _ in ring:
        pass

    @pl.loop(0, 4)
    def _(i):
        for j in range(4):
            for acc, pos, arrived in ((acc_a, x, rx_a), (acc_b, y, rx_b)):
                acc[pos, i, j] = (
                    acc[pos, i, j].astype(F32) + arrived[0, i, j].astype(F32) + arrived[1, i, j].astype(F32)
                ).astype(BF)

    def nothing(d):
        return None

    ring = ring_reduce(
        [("gz", y, acc_a.at[x], tr_c, rx_c, nothing), ("gx_0", x, acc_b.at[y], tr_d, rx_d, nothing)]
    )
    next(ring)
    fill(early, 2)
    next(ring)
    for _ in gather_x:
        pass
    fill(early, 1)
    for _ in ring:
        pass
    for j in range(4):
        zb[j] = (acc_a[x, y, j].astype(F32) + rx_c[0, j].astype(F32) + rx_c[1, j].astype(F32)).astype(BF)
        zb[4 + j] = (acc_b[y, x, j].astype(F32) + rx_d[0, j].astype(F32) + rx_d[1, j].astype(F32)).astype(BF)

    zc = [send(zb.at[(z + d) % 8], zr.at[d - 1], {"gy": (z + d) % 8}) for d in range(1, 8)]
    fill(late, 3)
    for copy in zc:
        copy.wait_recv()
    total = zb[z].astype(F32)
    for d in range(7):
        total = total + zr[d].astype(F32)
    domain = unpack(total).astype(BF)
    coupled = dot(domain, x_sq[...])
    gc[x, c, z // 4, y, z % 4] = pack(coupled).astype(BF)

    for _ in gather(gc):
        fill(late, 1)

    stores = []
    for g in range(n // 8):

        @pl.loop(0, 4)
        def _(i):
            for u in range(2):
                at = 8 * g + 2 * i + u
                combined = (both(gc, at) - pq[at].astype(F32)).astype(BF)
                w_sq[u, 0:R, :] = dot(combined, s_sq[at]).astype(BF)
            for u in range(2):
                at = 8 * g + 2 * i + u
                result = jnp.where(far < (ranks[at] + 1) * RSTEP, base[at] + dot(st[at], w_sq[u]), 0.0)
                tmp[u, 0] = result[:, 0:128]
                tmp[u, 1] = result[:, 128:256]
            for u in range(2):
                p = 2 * i + u
                low = low_lanes(96)
                el, er, ol, oh = (tmp[u, j, pl.ds(e, 96, stride=2), :] for e in range(2) for j in range(2))
                ol, oh = pltpu.roll(ol, 64, 1), pltpu.roll(oh, 64, 1)
                lines[pl.ds(p, 96, stride=24), :] = el
                lines[pl.ds(8 + p, 96, stride=24), :] = jnp.where(low, er, ol)
                lines[pl.ds(16 + p, 96, stride=24), :] = jnp.where(low, ol, oh)

        @pl.loop(0, LINES // 12)
        def _(i):
            for u in range(12):
                at = i * 12 + u
                s_raw[8 * g : 8 * g + 8, pl.ds(pl.multiple_of(at * 128, 128), 128)] = lines[
                    pl.ds(pl.multiple_of(at * 8, 8), 8), :
                ].astype(BF)

        copy = pltpu.make_async_copy(s_raw.at[8 * g : 8 * g + 8], o_hbm.at[8 * g : 8 * g + 8], store_sem.at[g])
        copy.start()
        stores.append(copy)
    for copy in stores:
        copy.wait()
    for copy in started:
        copy.wait_send()


def body(pair_list, rank_bucket, amplitudes, intersects, integrals, exchange_blocks):
    n = amplitudes.shape[0]
    named = (pair_list[None] == jnp.arange(64, dtype=jnp.int32)[:, None, None]).any(axis=2)
    number = jnp.arange(n, dtype=jnp.int32)[None, :]
    low = jnp.min(jnp.where(named, number, n), axis=1)
    high = jnp.max(jnp.where(named, number, -1), axis=1)
    inv = jnp.stack([low, jnp.where(high > low, high, n)], axis=1).reshape(128)

    smem = pl.BlockSpec(memory_space=pltpu.SMEM)
    hbm = pl.BlockSpec(memory_space=pl.ANY)
    vmem = pl.BlockSpec(memory_space=pltpu.VMEM)
    tail = (CH, 128)
    return pl.pallas_call(
        lambda inv, ranks, pairs, t, s, v, xr, o, *rest: kernel(inv, ranks, t, s, v, xr, o, *rest[:-4], pairs, *rest[-4:]),
        in_specs=[smem, smem, smem, hbm, hbm, hbm, vmem],
        out_specs=hbm,
        out_shape=jax.ShapeDtypeStruct((n, R * R), BF),
        scratch_shapes=[
            pltpu.VMEM((n, R * R), BF),
            pltpu.VMEM((n, R * R), BF),
            pltpu.VMEM((n, R * R), BF),
            pltpu.VMEM((LINES * 8, 128), F32),
            pltpu.VMEM((LINES, 128), F32),
            pltpu.VMEM((2, 2, R, 128), F32),
            pltpu.VMEM((n, W, W), BF),
            pltpu.VMEM((n, W, W), BF),
            pltpu.VMEM((2, W, W), BF),
            pltpu.VMEM((W, W), BF),
            pltpu.VMEM((2, W, W), BF),
            pltpu.VMEM((n, R, W), BF),
            pltpu.VMEM((n, R, W), BF),
            pltpu.VMEM((n, R, W), F32),
            pltpu.VMEM((n + 1, 4) + tail, BF),
            pltpu.VMEM((4, 2, 2, 4, 4) + tail, BF),
            pltpu.VMEM((4, 2, 2, 4, 4) + tail, BF),
            *[pltpu.VMEM((4, 4, 4) + tail, BF)] * 6,
            *[pltpu.VMEM((2, 2, 4) + tail, BF), pltpu.VMEM((2, 4, 4) + tail, BF)] * 2,
            *[pltpu.VMEM((2, 2) + tail, BF), pltpu.VMEM((2, 4) + tail, BF)] * 2,
            pltpu.VMEM((8,) + tail, BF),
            pltpu.VMEM((7,) + tail, BF),
            pltpu.SemaphoreType.DMA((3, n // 8)),
            pltpu.SemaphoreType.DMA((n // 8,)),
            pltpu.SemaphoreType.DMA((112,)),
            pltpu.SemaphoreType.DMA((112,)),
        ],
        compiler_params=pltpu.CompilerParams(collective_id=0, has_side_effects=True, vmem_limit_bytes=67043328),
    )(inv, rank_bucket, pair_list.reshape(2 * n), amplitudes, intersects, integrals, exchange_blocks)


def solution(mesh):
    torus = Mesh(mesh.devices.reshape(4, 2, mesh.shape["gy"], mesh.shape["gz"]), GX_GY_GZ)
    return jax.shard_map(
        body,
        mesh=torus,
        in_specs=(
            P(GX_GY_GZ, None),
            P(GX_GY_GZ),
            P(GX_GY_GZ, None),
            P(GX_GY_GZ, None),
            P(GX_GY_GZ, None),
            P(GX_GY, None),
        ),
        out_specs=P(GX_GY_GZ, None),
        check_vma=False,
    )
```

```python
import itertools
import math

import jax
import jax.numpy as jnp
from jax import lax
from jax.experimental import pallas as pl
from jax.experimental.pallas import tpu as pltpu
from jax.sharding import Mesh
from jax.sharding import PartitionSpec as P

RSTEP = 64
R = 192
W = 256
Q = 48
CH = 72
LINES = R * R // 128
UNROLL = 4
OUT, INTO = 11, 96
GX_GY = ("gx_0", "gx_1", "gy")
GX_GY_GZ = ("gx_0", "gx_1", "gy", "gz")
MESH = pl.DeviceIdType.MESH
BF = jnp.bfloat16
F32 = jnp.float32


def pack(v):
    right = v[:, 128:256]
    return jnp.concatenate([v[:, 0:128], right[0:24] + pltpu.roll(right[24:48], 64, 1)], axis=0)


def unpack(c):
    right = jnp.concatenate([c[48:72], pltpu.roll(c[48:72], 64, 1)], axis=0)
    return jnp.concatenate([c[0:48], right], axis=1)


def dot(a, b, ca=1, cb=0):
    return lax.dot_general(a, b, (((ca,), (cb,)), ((), ())), preferred_element_type=F32)


def low_lanes(n):
    return lax.broadcasted_iota(jnp.int32, (n, 128), 1) < 64


def even_odd(l0, l1, l2):
    low = low_lanes(l0.shape[0])
    t1, t2 = pltpu.roll(l1, 64, 1), pltpu.roll(l2, 64, 1)
    return (l0, jnp.where(low, l1, 0.0)), (jnp.where(low, t1, t2), jnp.where(low, t2, 0.0))


def kernel(
    pairs_hbm, ranks_hbm, t_hbm, s_hbm, v_hbm, x_hbm, o_ref,
    s_raw, t_raw, v_raw, x_raw, lines, lines2, xl, tmp, s_sq, m_sq, v_sq, x_sq, w_sq, st, pq, base, pp,
    gc, gx, sb_a, sb_b, rc_a, rc_b, acc_a, acc_b, tr_a, rx_a, tr_b, rx_b, tr_c, rx_c, tr_d, rx_d, zb, zr,
    inv_v, inv, pairs, ranks, load_sem, store_sem, small_sem, send_sem, recv_sem,
):
    n = s_raw.shape[0]
    groups = n // 8
    x, c, z, y = (lax.axis_index(a) for a in GX_GY_GZ)
    barrier = pltpu.get_barrier_semaphore()
    peers = [{"gx_1": 1 - c}]
    peers += [{"gx_0": (x + d) % 4} for d in (1, 2, 3)]
    peers += [{"gz": (y + d) % 4} for d in (1, 3)]
    peers += [{"gy": (z + d) % 8} for d in range(1, 8)]
    for who in peers:
        pl.semaphore_signal(barrier, inc=1, device_id=who, device_id_type=MESH)

    small = []
    for i, (src, dst) in enumerate(((ranks_hbm, ranks), (pairs_hbm, pairs), (x_hbm, x_raw))):
        copy = pltpu.make_async_copy(src, dst, small_sem.at[i])
        copy.start()
        small.append(copy)
    loads = {}
    for i, g in [(i, g) for g in range(groups) for i in (0, 1)] + [(2, g) for g in range(groups)]:
        src, dst = ((s_hbm, s_raw), (t_hbm, t_raw), (v_hbm, v_raw))[i]
        copy = pltpu.make_async_copy(src.at[8 * g : 8 * g + 8], dst.at[8 * g : 8 * g + 8], load_sem.at[i, g])
        copy.start()
        loads[i, g] = copy

    leaving, arriving = {}, {}

    def slot(groups, name):
        groups.setdefault(name, [len(groups), 0])
        return groups[name]

    def send(src, dst, axis, at, out, into):
        size = math.prod(src.shape[:-2])
        for groups, name in ((leaving, out), (arriving, into)):
            slot(groups, name)[1] += size
        copy = pltpu.make_async_remote_copy(
            src_ref=src,
            dst_ref=dst,
            send_sem=send_sem.at[leaving[out][0]],
            recv_sem=recv_sem.at[arriving[into][0]],
            device_id={axis: at},
            device_id_type=MESH,
        )
        copy.start()

    def await_all(sem, size):
        for dims in itertools.product((4, 3, 2, 1), (2, 1), (2, 1), (4, 3, 2, 1), (4, 3, 2, 1)):
            if math.prod(dims) == size:
                ref = gc.at[tuple(slice(0, d) for d in dims)]
                break
        else:
            assert size == zr.shape[0]
            ref = zr
        pltpu.make_async_copy(ref, ref, sem).wait()

    def arrived(into):
        await_all(recv_sem.at[arriving[into][0]], arriving[into][1])

    def to_lines(raws, g):
        @pl.loop(0, LINES // 12)
        def _(i):
            for u in range(12):
                at = i * 12 + u
                for raw, to in zip(raws, (lines, lines2)):
                    to[pl.ds(pl.multiple_of(at * 8, 8), 8), :] = raw[
                        8 * g : 8 * g + 8, pl.ds(pl.multiple_of(at * 128, 128), 128)
                    ].astype(F32)

    def halves(src, p):
        return even_odd(*(src[pl.ds(8 * i + p, 96, stride=24), :] for i in range(3)))

    def natural(src, p, u):
        for i, half in enumerate(halves(src, p)):
            for j in range(2):
                tmp[u, j, pl.ds(i, 96, stride=2), :] = half[j]
        return square(u)

    def skewed(count, *stages):
        for step in range(count + len(stages) - 1):
            for i, stage in enumerate(stages):
                if 0 <= step - i < count:
                    stage(step - i)

    def square(u):
        return jnp.concatenate([tmp[u, 0], tmp[u, 1]], axis=1)

    row = lax.broadcasted_iota(jnp.int32, (R, W), 0)
    col = lax.broadcasted_iota(jnp.int32, (R, W), 1)
    far = jnp.maximum(row, col)

    def project(g):
        loads[0, g].wait()
        loads[1, g].wait()
        to_lines((s_raw, t_raw), g)

        @pl.loop(0, 8 // UNROLL)
        def _(i):
            half = {}

            def reshaped(u):
                p = UNROLL * i + u
                at = 8 * g + p
                for k, part in enumerate(halves(lines, p)):
                    s_sq[at, 96 * k : 96 * k + 96, :] = jnp.concatenate(part, axis=1).astype(BF)
                s_sq[at, R:W, :] = jnp.zeros((W - R, W), BF)
                m_sq[at, 0:R, :] = jnp.where(far < (ranks[at] + 1) * RSTEP, natural(lines2, p, u), 0.0).astype(BF)
                m_sq[at, R:W, :] = jnp.zeros((W - R, W), BF)

            def left(u):
                at = 8 * g + UNROLL * i + u
                half[u] = dot(s_sq[at, 0:R, :], m_sq[at]).astype(BF)

            def right(u):
                at = 8 * g + UNROLL * i + u
                full = dot(half.pop(u), s_sq[at], 1, 1).astype(BF)
                pq[at] = full
                full = full.astype(F32)
                for q in range(4):
                    pp[at, q] = pack(full[Q * q : Q * q + Q]).astype(BF)

            skewed(UNROLL, reshaped, left, right)

    small[0].wait()
    project(0)

    small[2].wait()

    @pl.loop(0, LINES // 8)
    def _(i):
        for u in range(8):
            xl[pl.ds(i * 8 + u, 1), :] = x_raw[0:1, pl.ds(pl.multiple_of((i * 8 + u) * 128, 128), 128)].astype(F32)

    even, odd = even_odd(*(xl[pl.ds(i, 96, stride=3), :] for i in range(3)))
    at = lax.broadcasted_iota(jnp.int32, (W, W), 1)
    to = jnp.where(at < 96, 2 * at, jnp.where(at < R, 2 * at - (R - 1), -1))
    turn = (lax.broadcasted_iota(jnp.int32, (W, W), 0) == to).astype(F32).astype(BF)
    for i, half in enumerate((even, odd)):
        x_sq[96 * i : 96 * i + 96, :] = dot(jnp.concatenate(half, axis=1).astype(BF), turn).astype(BF)
    x_sq[R:W, :] = jnp.zeros((W - R, W), BF)
    for q in range(4):
        gx[0, c, z, q] = pack(x_sq[Q * q : Q * q + Q, :].astype(F32)).astype(BF)
    for i in range(UNROLL):
        w_sq[i, R:W, :] = jnp.zeros((W - R, W), BF)
    for i in range(2):
        v_sq[i, R:W, :] = jnp.zeros((W - R, W), BF)
    pp[n] = jnp.zeros((4, CH, 128), BF)

    small[1].wait()
    lane = lax.broadcasted_iota(jnp.int32, (1, 128), 1)
    low = jnp.full((1, 128), n, jnp.int32)
    high = low
    for p in range(n):
        named = (lane == pairs[0, p]) | (lane == pairs[1, p])
        high = jnp.where(named & (low < n), p, high)
        low = jnp.where(named & (low == n), p, low)
    inv_v[0:1, :] = low
    inv_v[1:2, :] = high
    to_inv = pltpu.make_async_copy(inv_v, inv, small_sem.at[3])
    to_inv.start()

    pl.semaphore_wait(barrier, len(peers))

    def gather_blocks():
        pieces = ((slice(0, 1),) * 2, (slice(1, 2), slice(2, 3)), (slice(3, 4),) * 2)

        def ref(i, d):
            return gx.at[pieces[i][0].start : pieces[i][1].stop, c, (z + d) % 8]

        def hop(i, step):
            if step > 1:
                arrived(("xu", i, step - 1))
            up = ref(i, 9 - step)
            if step == 4:
                up = gx.at[pieces[i][0], c, (z + 5) % 8]
                up = up if i == 1 else up.at[:, 0:2]
            into = ("x4", i) if step == 4 else ("xu", i, step)
            send(up, up, "gy", (z + 1) % 8, "x4" if step == 4 else "xz", into)
            if step > 1:
                arrived(("xd", i, step - 1))
            down = ref(i, step - 1)
            if step == 4:
                down = gx.at[pieces[i][1], c, (z + 3) % 8]
                down = down if i == 1 else down.at[:, 2:4]
            into = ("x4", i) if step == 4 else ("xd", i, step)
            send(down, down, "gy", (z + 7) % 8, "x4" if step == 4 else "xz", into)
            if i == 2:
                for d in {(9 - step) % 8, step - 1}:
                    across_x(d)

        def across_x(d):
            send(gx.at[:, c, (z + d) % 8], gx.at[:, c, (z + d) % 8], "gx_1", 1 - c, "xc", "xc")

        own = gx.at[0, c, z]
        send(own, gx.at[2, c, z], "gx_0", (x + 1) % 4, "xx", "x-")
        send(own, gx.at[1, c, z], "gx_0", (x + 3) % 4, "xx", "x+")
        hop(0, 1)
        yield
        hop(0, 2)
        arrived("x-")
        send(gx.at[2, c, z, 0:2], gx.at[3, c, z, 0:2], "gx_0", (x + 1) % 4, "z", "x2")
        arrived("x+")
        send(gx.at[1, c, z, 2:4], gx.at[3, c, z, 2:4], "gx_0", (x + 3) % 4, "z", "x2")
        hop(1, 1)
        yield
        hop(0, 3)
        arrived("x2")
        hop(2, 1)
        yield
        for i, step in ((1, 2), (0, 4), (2, 2), (1, 3), (2, 3), (1, 4), (2, 4)):
            hop(i, step)
            yield
        for i in range(3):
            arrived(("x4", i))
        across_x(4)
        yield
        arrived("xc")

    gather_x = gather_blocks()
    next(gather_x)
    project(1)
    project(2)
    next(gather_x)
    for g in range(3, groups):
        project(g)

    def transposes(g):
        @pl.loop(0, 8)
        def _(p):
            st[8 * g + p] = s_sq[8 * g + p].T[0:R]

    def local(g, part):
        if part == 0:
            loads[2, g].wait()
            to_lines((v_raw,), g)

        @pl.loop(2 * part, 2 * part + 2)
        def _(i):
            for u in range(2):
                v_sq[u, 0:R, :] = natural(lines, 2 * i + u, u).astype(BF)
            for u in range(2):
                at = 8 * g + 2 * i + u
                base[at] = square(u) + dot(m_sq[at, 0:R, :], v_sq[u])

    def of_coupled(k, q):
        return gc[k // 16, k // 8 % 2, k // 4 % 2, q, k % 4].astype(F32)

    def of_exchange(k, q):
        d = (k // 16 + 4 - x) % 4
        return gx[jnp.where(d < 2, d, 5 - d), k // 8 % 2, k % 8, q].astype(F32)

    def both(of, at):
        k0, k1 = pairs[0, at], pairs[1, at]
        return jnp.concatenate([unpack(of(k0, q) + of(k1, q)) for q in range(4)], axis=0)

    def own_terms(g):
        @pl.loop(0, 4)
        def _(i):
            for u in range(2):
                at = 8 * g + 2 * i + u
                w_sq[u, 0:R, :] = both(of_exchange, at).astype(BF)
            for u in range(2):
                at = 8 * g + 2 * i + u
                pq[at] = dot(pq[at], w_sq[u]).astype(BF)

    early = [lambda g=g, part=part: local(g, part) for g in range(groups) for part in range(2)] + [lambda g=g: transposes(g) for g in range(groups)]
    late = [lambda g=g: own_terms(g) for g in range(groups)]

    def fill(work, count=1):
        for _ in range(count):
            if work:
                work.pop(0)()

    to_inv.wait()
    order = (2, 1, 3, 0)

    def ends(k, q):
        return pp[inv[0, k], q].astype(F32) + pp[inv[1, k], q].astype(F32)

    def each_a(q, c, put):
        @pl.loop(0, 4)
        def _(xx):
            for j in range(4):
                put(xx, q, j, ends(xx * 16 + c * 8 + j, q))

    def each_b(xx, c, put):
        @pl.loop(0, 4)
        def _(q):
            for j in range(4):
                put(q, xx, j, ends(xx * 16 + c * 8 + 4 + j, q))

    def put_in(ref, also=None):
        def put(t1, t2, j, value):
            if also is not None:
                value = value + also[t1, t2, j].astype(F32)
            ref[t1, t2, j] = value.astype(BF)

        return put

    for d in order:
        at = (y + d) % 4
        each_a(at, 1 - c, put_in(sb_a))
        send(sb_a.at[:, at], rc_a.at[:, at], "gx_1", 1 - c, "core", ("a", d))
        at = (x + d) % 4
        each_b(at, 1 - c, put_in(sb_b))
        send(sb_b.at[:, at], rc_b.at[:, at], "gx_1", 1 - c, "core", ("b", d))
    next(gather_x)

    def ready_a(d):
        arrived(("a", d))
        each_a((y + d) % 4, c, put_in(acc_a, rc_a))

    def ready_b(d):
        arrived(("b", d))
        each_b((x + d) % 4, c, put_in(acc_b, rc_b))

    def add(dst, *srcs):
        for j in range(dst.shape[0]):
            value = dst[j].astype(F32)
            for src in srcs:
                value = value + src[j].astype(F32)
            dst[j] = value.astype(BF)

    class Reduce:
        def __init__(self, name, axis1, p1, axis2, p2, acc, tr1, rx1, tr2, rx2, ready):
            self.name, self.axis1, self.p1, self.axis2, self.p2 = name, axis1, p1, axis2, p2
            self.acc, self.tr1, self.rx1, self.tr2, self.rx2, self.ready = acc, tr1, rx1, tr2, rx2, ready

        def sub(self, d1, d2):
            return self.acc.at[(self.p1 + d1) % 4, (self.p2 + d2) % 4]

        def first(self, turn, src, dst, *into):
            send(src, dst, self.axis1, (self.p1 + turn) % 4, "ring1", (self.name, *into))

        def second(self, turn, src, dst, *into):
            send(src, dst, self.axis2, (self.p2 + turn) % 4, "ring2", (self.name, *into))

        def s1(self, d):
            self.ready(d)
            k = order.index(d)
            self.first(1, self.sub(2, d).at[0:2], self.tr1.at[0, k], "u", d)
            self.first(3, self.sub(2, d).at[2:4], self.tr1.at[1, k], "d", d)
            self.first(1, self.sub(1, d).at[2:4], self.rx1.at[0, k, 2:4], "r", d)
            self.first(3, self.sub(3, d).at[0:2], self.rx1.at[1, k, 0:2], "r", d)

        def s2(self, d):
            k = order.index(d)
            arrived((self.name, "u", d))
            add(self.sub(1, d).at[0:2], self.tr1.at[0, k])
            self.first(1, self.sub(1, d).at[0:2], self.rx1.at[0, k, 0:2], "r", d)
            arrived((self.name, "d", d))
            add(self.sub(3, d).at[2:4], self.tr1.at[1, k])
            self.first(3, self.sub(3, d).at[2:4], self.rx1.at[1, k, 2:4], "r", d)

        def s3(self, d):
            k = order.index(d)
            arrived((self.name, "r", d))
            mine = self.sub(0, d)
            add(mine, self.rx1.at[0, k], self.rx1.at[1, k])
            if d == 2:
                self.second(1, mine.at[0:2], self.tr2.at[0], "u2")
                self.second(3, mine.at[2:4], self.tr2.at[1], "d2")
            if d == 1:
                self.second(1, mine.at[2:4], self.rx2.at[0, 2:4], "r2")
            if d == 3:
                self.second(3, mine.at[0:2], self.rx2.at[1, 0:2], "r2")

        def u3(self):
            arrived((self.name, "u2"))
            add(self.sub(0, 1).at[0:2], self.tr2.at[0])
            self.second(1, self.sub(0, 1).at[0:2], self.rx2.at[0, 0:2], "r2")
            arrived((self.name, "d2"))
            add(self.sub(0, 3).at[2:4], self.tr2.at[1])
            self.second(3, self.sub(0, 3).at[2:4], self.rx2.at[1, 2:4], "r2")

        def u4(self, at):
            arrived((self.name, "r2"))
            mine = self.sub(0, 0)
            for j in range(4):
                zb[at + j] = (mine[j].astype(F32) + self.rx2[0, j].astype(F32) + self.rx2[1, j].astype(F32)).astype(BF)

    both_rings = (
        Reduce("A", "gx_0", x, "gz", y, acc_a, tr_a, rx_a, tr_c, rx_c, ready_a),
        Reduce("B", "gz", y, "gx_0", x, acc_b, tr_b, rx_b, tr_d, rx_d, ready_b),
    )
    for d in order:
        for r in both_rings:
            r.s1(d)
    fill(early)
    next(gather_x)
    for i, d in enumerate(order):
        for r in both_rings:
            r.s2(d)
        if i < 3:
            fill(early)
            next(gather_x)
    for i, d in enumerate(order):
        for r in both_rings:
            r.s3(d)
        if i == 2:
            next(gather_x)
    for r in both_rings:
        r.u3()
    next(gather_x)
    for i, r in enumerate(both_rings):
        r.u4(4 * i)

    for d in (4, 3, 5, 2, 6, 1, 7):
        send(zb.at[(z + d) % 8], zr.at[d - 1], "gy", (z + d) % 8, "z", "z")
    fill(early, 1)
    next(gather_x)
    fill(early, 3)
    arrived("z")
    total = zb[z].astype(F32)
    for d in range(7):
        total = total + zr[d].astype(F32)
    domain = unpack(total).astype(BF)
    coupled = dot(domain, x_sq[...])
    gc[x, c, z // 4, y, z % 4] = pack(coupled).astype(BF)

    def across(ref):
        send(ref, ref, "gx_1", 1 - c, "over", "over")

    class Gather:
        def __init__(self, name, axis2, p2, axis3, p3, sub):
            self.name, self.axis2, self.p2, self.axis3, self.p3 = name, axis2, p2, axis3, p3
            self.at = sub

        def sub(self, d3, d2):
            return self.at((self.p3 + d3) % 4, (self.p2 + d2) % 4)

        def turn2(self, ref, d, *into):
            send(ref, ref, self.axis2, (self.p2 + d) % 4, "turn2", ("g" + self.name, *into))

        def turn3(self, ref, d, *into):
            send(ref, ref, self.axis3, (self.p3 + d) % 4, "turn3", ("g" + self.name, *into))

        def arrived(self, *into):
            arrived(("g" + self.name, *into))

        def spread(self, d):
            ref = self.sub(0, d)
            self.turn3(ref, 1, "u", d)
            self.turn3(ref, 3, "d", d)
            across(ref)

        def t0(self):
            ref = self.sub(0, 0)
            self.turn2(ref, 1, "u")
            self.turn2(ref, 3, "d")
            self.spread(0)

        def t1(self):
            self.arrived("u")
            self.turn2(self.sub(0, 3).at[0:2], 1, "far")
            self.arrived("d")
            self.turn2(self.sub(0, 1).at[2:4], 3, "far")
            self.spread(3)
            self.spread(1)

        def t3(self):
            self.arrived("far")
            self.spread(2)

        def on(self, d):
            self.arrived("u", d)
            ref = self.sub(3, d)
            self.turn3(ref.at[0:2], 1, "far", d)
            across(ref)
            self.arrived("d", d)
            ref = self.sub(1, d)
            self.turn3(ref.at[2:4], 3, "far", d)
            across(ref)

        def last(self, d):
            self.arrived("far", d)
            across(self.sub(2, d))

    own = gc.at[x, c, z // 4, y, z % 4]
    for d in (4, 3, 5, 2, 6, 1, 7):
        send(own, own, "gy", (z + d) % 8, "z", "gz")
    fill(early, 12)
    next(gather_x)
    arrived("gz")
    both_rings = (
        Gather("A", "gz", y, "gx_0", x, lambda i3, i2: gc.at[i3, c, 0, i2]),
        Gather("B", "gx_0", x, "gz", y, lambda i3, i2: gc.at[i2, c, 1, i3]),
    )
    for r in both_rings:
        r.t0()
    for _ in gather_x:
        pass
    fill(late)
    for r in both_rings:
        r.t1()
    for r in both_rings:
        r.on(0)
    for r in both_rings:
        r.t3()
    fill(late)
    for d in (3, 1):
        for r in both_rings:
            r.on(d)
    for r in both_rings:
        r.last(0)
    fill(late)
    for r in both_rings:
        r.on(2)
    fill(late)
    for d in (3, 1, 2):
        for r in both_rings:
            r.last(d)
    arrived("over")

    stores = []
    for g in range(groups):
        @pl.loop(0, 8 // UNROLL)
        def _(i):
            def right(u):
                at = 8 * g + UNROLL * i + u
                combined = (both(of_coupled, at) - pq[at].astype(F32)).astype(BF)
                w_sq[u, 0:R, :] = dot(combined, s_sq[at]).astype(BF)

            def left(u):
                at = 8 * g + UNROLL * i + u
                result = jnp.where(far < (ranks[at] + 1) * RSTEP, base[at] + dot(st[at], w_sq[u]), 0.0)
                tmp[u, 0] = result[:, 0:128]
                tmp[u, 1] = result[:, 128:256]

            def flat(u):
                p = UNROLL * i + u
                low = low_lanes(96)
                el, er, ol, oh = (tmp[u, j, pl.ds(e, 96, stride=2), :] for e in range(2) for j in range(2))
                ol, oh = pltpu.roll(ol, 64, 1), pltpu.roll(oh, 64, 1)
                lines[pl.ds(p, 96, stride=24), :] = el
                lines[pl.ds(8 + p, 96, stride=24), :] = jnp.where(low, er, ol)
                lines[pl.ds(16 + p, 96, stride=24), :] = jnp.where(low, ol, oh)

            skewed(UNROLL, right, left, flat)

        @pl.loop(0, LINES // 12)
        def _(i):
            for u in range(12):
                at = i * 12 + u
                s_raw[8 * g : 8 * g + 8, pl.ds(pl.multiple_of(at * 128, 128), 128)] = lines[
                    pl.ds(pl.multiple_of(at * 8, 8), 8), :
                ].astype(BF)

        copy = pltpu.make_async_copy(s_raw.at[8 * g : 8 * g + 8], o_ref.at[8 * g : 8 * g + 8], store_sem.at[g])
        copy.start()
        stores.append(copy)

    for copy in stores:
        copy.wait()
    assert len(leaving) == OUT and len(arriving) == INTO
    for index, size in leaving.values():
        await_all(send_sem.at[index], size)


def body(pair_list, rank_bucket, amplitudes, intersects, integrals, exchange_blocks):
    n = amplitudes.shape[0]
    hbm = pl.BlockSpec(memory_space=pl.ANY)
    tail = (CH, 128)
    return pl.pallas_call(
        kernel,
        in_specs=[hbm] * 6,
        out_specs=hbm,
        out_shape=jax.ShapeDtypeStruct((n, R * R), BF),
        scratch_shapes=[
            *[pltpu.VMEM((n, R * R), BF)] * 3,
            pltpu.VMEM((1, R * R), BF),
            *[pltpu.VMEM((LINES * 8, 128), F32)] * 2,
            pltpu.VMEM((LINES, 128), F32),
            pltpu.VMEM((UNROLL, 2, R, 128), F32),
            pltpu.VMEM((n, W, W), BF),
            pltpu.VMEM((n, W, W), BF),
            pltpu.VMEM((2, W, W), BF),
            pltpu.VMEM((W, W), BF),
            pltpu.VMEM((UNROLL, W, W), BF),
            pltpu.VMEM((n, R, W), BF),
            pltpu.VMEM((n, R, W), BF),
            pltpu.VMEM((n, R, W), F32),
            pltpu.VMEM((n + 1, 4) + tail, BF),
            pltpu.VMEM((4, 2, 2, 4, 4) + tail, BF),
            pltpu.VMEM((4, 2, 8, 4) + tail, BF),
            *[pltpu.VMEM((4, 4, 4) + tail, BF)] * 6,
            *[pltpu.VMEM((2, 4, 2) + tail, BF), pltpu.VMEM((2, 4, 4) + tail, BF)] * 2,
            *[pltpu.VMEM((2, 2) + tail, BF), pltpu.VMEM((2, 4) + tail, BF)] * 2,
            pltpu.VMEM((8,) + tail, BF),
            pltpu.VMEM((7,) + tail, BF),
            pltpu.VMEM((2, 128), jnp.int32),
            pltpu.SMEM((2, 128), jnp.int32),
            pltpu.SMEM((2, n), jnp.int32),
            pltpu.SMEM((n,), jnp.int32),
            pltpu.SemaphoreType.DMA((3, n // 8)),
            pltpu.SemaphoreType.DMA((n // 8,)),
            pltpu.SemaphoreType.DMA((4,)),
            pltpu.SemaphoreType.DMA((OUT,)),
            pltpu.SemaphoreType.DMA((INTO,)),
        ],
        compiler_params=pltpu.CompilerParams(collective_id=0, has_side_effects=True, vmem_limit_bytes=58 * 2**20),
    )(pair_list.T, rank_bucket, amplitudes, intersects, integrals, exchange_blocks)


def solution(mesh):
    torus = Mesh(mesh.devices.reshape(4, 2, mesh.shape["gy"], mesh.shape["gz"]), GX_GY_GZ)
    return jax.shard_map(
        body,
        mesh=torus,
        in_specs=(
            P(GX_GY_GZ, None),
            P(GX_GY_GZ),
            P(GX_GY_GZ, None),
            P(GX_GY_GZ, None),
            P(GX_GY_GZ, None),
            P(GX_GY, None),
        ),
        out_specs=P(GX_GY_GZ, None),
        check_vma=False,
    )
```

```python
import itertools
import math

import jax
import jax.numpy as jnp
from jax import lax
from jax.experimental import pallas as pl
from jax.experimental.pallas import tpu as pltpu
from jax.sharding import Mesh
from jax.sharding import PartitionSpec as P

RSTEP = 64
R = 192
W = 256
Q = 48
CH = 72
LINES = R * R // 128
UNROLL = 8
OUT, INTO = 11, 96
GX_GY = ("gx_0", "gx_1", "gy")
GX_GY_GZ = ("gx_0", "gx_1", "gy", "gz")
MESH = pl.DeviceIdType.MESH
BF = jnp.bfloat16
F32 = jnp.float32


def pack(v):
    right = v[:, 128:256]
    return jnp.concatenate([v[:, 0:128], right[0:24] + pltpu.roll(right[24:48], 64, 1)], axis=0)


def unpack(c):
    right = jnp.concatenate([c[48:72], pltpu.roll(c[48:72], 64, 1)], axis=0)
    return jnp.concatenate([c[0:48], right], axis=1)


def dot(a, b, ca=1, cb=0):
    return lax.dot_general(a, b, (((ca,), (cb,)), ((), ())), preferred_element_type=F32)


def low_lanes(n):
    return lax.broadcasted_iota(jnp.int32, (n, 128), 1) < 64


def even_odd(l0, l1, l2):
    low = low_lanes(l0.shape[0])
    t1, t2 = pltpu.roll(l1, 64, 1), pltpu.roll(l2, 64, 1)
    return (l0, jnp.where(low, l1, 0.0)), (jnp.where(low, t1, t2), jnp.where(low, t2, 0.0))


def kernel(
    pairs_hbm, ranks_hbm, t_hbm, s_hbm, v_hbm, x_hbm, o_ref,
    s_raw, t_raw, x_raw, lines, lines2, xl, tmp, s_sq, m_sq, v_sq, x_sq, w_sq, pq, base, pp,
    gc, gx, sb_a, sb_b, rc_a, rc_b, acc_a, acc_b, tr_a, rx_a, tr_b, rx_b, tr_c, rx_c, tr_d, rx_d, zb, zr,
    inv_v, inv, pairs, ranks, load_sem, small_sem, send_sem, recv_sem,
):
    n = s_raw.shape[0]
    groups = n // 8
    x, c, z, y = (lax.axis_index(a) for a in GX_GY_GZ)
    barrier = pltpu.get_barrier_semaphore()
    peers = [{"gx_1": 1 - c}]
    peers += [{"gx_0": (x + d) % 4} for d in (1, 2, 3)]
    peers += [{"gz": (y + d) % 4} for d in (1, 3)]
    peers += [{"gy": (z + d) % 8} for d in range(1, 8)]
    for who in peers:
        pl.semaphore_signal(barrier, inc=1, device_id=who, device_id_type=MESH)

    small = []
    for i, (src, dst) in enumerate(((ranks_hbm, ranks), (pairs_hbm, pairs), (x_hbm, x_raw))):
        copy = pltpu.make_async_copy(src, dst, small_sem.at[i])
        copy.start()
        small.append(copy)
    loads = {}
    def load(i, g):
        src, dst = ((s_hbm, s_raw), (t_hbm, t_raw), (v_hbm, s_raw))[i]
        copy = pltpu.make_async_copy(src.at[8 * g : 8 * g + 8], dst.at[8 * g : 8 * g + 8], load_sem.at[i, g])
        copy.start()
        loads[i, g] = copy

    for g in range(groups):
        load(0, g)
        load(1, g)

    leaving, arriving = {}, {}

    def slot(groups, name):
        groups.setdefault(name, [len(groups), 0])
        return groups[name]

    def send(src, dst, axis, at, out, into):
        size = math.prod(src.shape[:-2])
        for groups, name in ((leaving, out), (arriving, into)):
            slot(groups, name)[1] += size
        copy = pltpu.make_async_remote_copy(
            src_ref=src,
            dst_ref=dst,
            send_sem=send_sem.at[leaving[out][0]],
            recv_sem=recv_sem.at[arriving[into][0]],
            device_id={axis: at},
            device_id_type=MESH,
        )
        copy.start()

    def await_all(sem, size):
        for dims in itertools.product((4, 3, 2, 1), (2, 1), (2, 1), (4, 3, 2, 1), (4, 3, 2, 1)):
            if math.prod(dims) == size:
                ref = gc.at[tuple(slice(0, d) for d in dims)]
                break
        else:
            assert size == zr.shape[0]
            ref = zr
        pltpu.make_async_copy(ref, ref, sem).wait()

    def arrived(into):
        await_all(recv_sem.at[arriving[into][0]], arriving[into][1])

    def to_lines(raws, g):
        @pl.loop(0, LINES // 36)
        def _(i):
            for u in range(36):
                at = i * 36 + u
                for raw, to in zip(raws, (lines, lines2)):
                    to[pl.ds(pl.multiple_of(at * 8, 8), 8), :] = raw[
                        8 * g : 8 * g + 8, pl.ds(pl.multiple_of(at * 128, 128), 128)
                    ].astype(F32)

    def halves(src, p):
        return even_odd(*(src[pl.ds(8 * i + p, 96, stride=24), :] for i in range(3)))

    def natural(src, p, u):
        for i, half in enumerate(halves(src, p)):
            for j in range(2):
                tmp[u, j, pl.ds(i, 96, stride=2), :] = half[j]
        return square(u)

    def skewed(count, *stages):
        for step in range(count + len(stages) - 1):
            for i, stage in enumerate(stages):
                if 0 <= step - i < count:
                    stage(step - i)

    def square(u):
        return jnp.concatenate([tmp[u, 0], tmp[u, 1]], axis=1)

    row = lax.broadcasted_iota(jnp.int32, (R, W), 0)
    col = lax.broadcasted_iota(jnp.int32, (R, W), 1)
    far = jnp.maximum(row, col)

    def project(g):
        loads[0, g].wait()
        loads[1, g].wait()
        to_lines((s_raw, t_raw), g)
        load(2, g)
        if g == 0:
            small[0].wait()

        @pl.loop(0, 8 // UNROLL)
        def _(i):
            half = {}

            def reshaped(u):
                p = UNROLL * i + u
                at = 8 * g + p
                for k, part in enumerate(halves(lines, p)):
                    s_sq[at, 96 * k : 96 * k + 96, :] = jnp.concatenate(part, axis=1).astype(BF)
                s_sq[at, R:W, :] = jnp.zeros((W - R, W), BF)
                m_sq[at, 0:R, :] = jnp.where(far < (ranks[at] + 1) * RSTEP, natural(lines2, p, u), 0.0).astype(BF)
                m_sq[at, R:W, :] = jnp.zeros((W - R, W), BF)

            def left(u):
                at = 8 * g + UNROLL * i + u
                half[u] = dot(s_sq[at, 0:R, :], m_sq[at]).astype(BF)

            def right(u):
                at = 8 * g + UNROLL * i + u
                full = dot(half.pop(u), s_sq[at], 1, 1).astype(BF)
                pq[at] = full
                full = full.astype(F32)
                for q in range(4):
                    pp[at, q] = pack(full[Q * q : Q * q + Q]).astype(BF)

            skewed(UNROLL, reshaped, left, right)

    project(0)

    small[2].wait()

    @pl.loop(0, LINES // 8)
    def _(i):
        for u in range(8):
            xl[pl.ds(i * 8 + u, 1), :] = x_raw[0:1, pl.ds(pl.multiple_of((i * 8 + u) * 128, 128), 128)].astype(F32)

    even, odd = even_odd(*(xl[pl.ds(i, 96, stride=3), :] for i in range(3)))
    at = lax.broadcasted_iota(jnp.int32, (W, W), 1)
    to = jnp.where(at < 96, 2 * at, jnp.where(at < R, 2 * at - (R - 1), -1))
    turn = (lax.broadcasted_iota(jnp.int32, (W, W), 0) == to).astype(F32).astype(BF)
    for i, half in enumerate((even, odd)):
        x_sq[96 * i : 96 * i + 96, :] = dot(jnp.concatenate(half, axis=1).astype(BF), turn).astype(BF)
    x_sq[R:W, :] = jnp.zeros((W - R, W), BF)
    for q in range(4):
        gx[0, c, z, q] = pack(x_sq[Q * q : Q * q + Q, :].astype(F32)).astype(BF)
    for i in range(UNROLL):
        w_sq[i, R:W, :] = jnp.zeros((W - R, W), BF)
    for i in range(2):
        v_sq[i, R:W, :] = jnp.zeros((W - R, W), BF)
    pp[n] = jnp.zeros((4, CH, 128), BF)

    small[1].wait()
    lane = lax.broadcasted_iota(jnp.int32, (1, 128), 1)
    low = jnp.full((1, 128), n, jnp.int32)
    high = low
    for p in range(n):
        named = (lane == pairs[0, p]) | (lane == pairs[1, p])
        high = jnp.where(named & (low < n), p, high)
        low = jnp.where(named & (low == n), p, low)
    inv_v[0:1, :] = low
    inv_v[1:2, :] = high
    to_inv = pltpu.make_async_copy(inv_v, inv, small_sem.at[3])
    to_inv.start()

    pl.semaphore_wait(barrier, len(peers))

    def gather_blocks():
        pieces = ((slice(0, 1),) * 2, (slice(1, 2), slice(2, 3)), (slice(3, 4),) * 2)

        def ref(i, d):
            return gx.at[pieces[i][0].start : pieces[i][1].stop, c, (z + d) % 8]

        def hop(i, step):
            if step > 1:
                arrived(("xu", i, step - 1))
            up = ref(i, 9 - step)
            if step == 4:
                up = gx.at[pieces[i][0], c, (z + 5) % 8]
                up = up if i == 1 else up.at[:, 0:2]
            into = ("x4", i) if step == 4 else ("xu", i, step)
            send(up, up, "gy", (z + 1) % 8, "x4" if step == 4 else "xz", into)
            if step > 1:
                arrived(("xd", i, step - 1))
            down = ref(i, step - 1)
            if step == 4:
                down = gx.at[pieces[i][1], c, (z + 3) % 8]
                down = down if i == 1 else down.at[:, 2:4]
            into = ("x4", i) if step == 4 else ("xd", i, step)
            send(down, down, "gy", (z + 7) % 8, "x4" if step == 4 else "xz", into)
            if i == 2:
                for d in {(9 - step) % 8, step - 1}:
                    across_x(d)

        def across_x(d):
            send(gx.at[:, c, (z + d) % 8], gx.at[:, c, (z + d) % 8], "gx_1", 1 - c, "xc", "xc")

        own = gx.at[0, c, z]
        send(own, gx.at[2, c, z], "gx_0", (x + 1) % 4, "xx", "x-")
        send(own, gx.at[1, c, z], "gx_0", (x + 3) % 4, "xx", "x+")
        hop(0, 1)
        yield
        hop(0, 2)
        arrived("x-")
        send(gx.at[2, c, z, 0:2], gx.at[3, c, z, 0:2], "gx_0", (x + 1) % 4, "z", "x2")
        arrived("x+")
        send(gx.at[1, c, z, 2:4], gx.at[3, c, z, 2:4], "gx_0", (x + 3) % 4, "z", "x2")
        hop(1, 1)
        yield
        hop(0, 3)
        arrived("x2")
        hop(2, 1)
        yield
        for i, step in ((1, 2), (0, 4), (2, 2), (1, 3), (2, 3), (1, 4), (2, 4)):
            hop(i, step)
            yield
        for i in range(3):
            arrived(("x4", i))
        across_x(4)
        yield
        arrived("xc")

    gather_x = gather_blocks()
    next(gather_x)
    project(1)
    project(2)
    for g in range(3, groups):
        project(g)
    next(gather_x)

    def transposes(g):
        @pl.loop(0, 8)
        def _(p):
            m_sq[8 * g + p, 0:R, :] = s_sq[8 * g + p].T[0:R]

    def local(g, part):
        if part == 0:
            loads[2, g].wait()
            to_lines((s_raw,), g)

        @pl.loop(2 * part, 2 * part + 2)
        def _(i):
            for u in range(2):
                v_sq[u, 0:R, :] = natural(lines, 2 * i + u, u).astype(BF)
            for u in range(2):
                at = 8 * g + 2 * i + u
                base[at] = square(u) + dot(m_sq[at, 0:R, :], v_sq[u])

    def of_coupled(k, q):
        return gc[k // 16, k // 8 % 2, k // 4 % 2, q, k % 4].astype(F32)

    def of_exchange(k, q):
        d = (k // 16 + 4 - x) % 4
        return gx[jnp.where(d < 2, d, 5 - d), k // 8 % 2, k % 8, q].astype(F32)

    def both(of, at):
        k0, k1 = pairs[0, at], pairs[1, at]
        return jnp.concatenate([unpack(of(k0, q) + of(k1, q)) for q in range(4)], axis=0)

    def own_terms(g):
        @pl.loop(0, 4)
        def _(i):
            for u in range(2):
                at = 8 * g + 2 * i + u
                w_sq[u, 0:R, :] = both(of_exchange, at).astype(BF)
            for u in range(2):
                at = 8 * g + 2 * i + u
                pq[at] = dot(pq[at], w_sq[u]).astype(BF)

    early = [lambda g=g, part=part: local(g, part) for g in range(groups) for part in range(2)] + [lambda g=g: transposes(g) for g in range(groups)]
    late = [lambda g=g: own_terms(g) for g in range(groups)]

    def fill(work, count=1):
        for _ in range(count):
            if work:
                work.pop(0)()

    to_inv.wait()
    order = (2, 1, 3, 0)

    def ends(k, q):
        return pp[inv[0, k], q].astype(F32) + pp[inv[1, k], q].astype(F32)

    def each_a(q, c, put):
        @pl.loop(0, 4)
        def _(xx):
            for j in range(4):
                put(xx, q, j, ends(xx * 16 + c * 8 + j, q))

    def each_b(xx, c, put):
        @pl.loop(0, 4)
        def _(q):
            for j in range(4):
                put(q, xx, j, ends(xx * 16 + c * 8 + 4 + j, q))

    def put_in(ref, also=None):
        def put(t1, t2, j, value):
            if also is not None:
                value = value + also[t1, t2, j].astype(F32)
            ref[t1, t2, j] = value.astype(BF)

        return put

    for d in order:
        at = (y + d) % 4
        each_a(at, 1 - c, put_in(sb_a))
        send(sb_a.at[:, at], rc_a.at[:, at], "gx_1", 1 - c, "core", ("a", d))
        at = (x + d) % 4
        each_b(at, 1 - c, put_in(sb_b))
        send(sb_b.at[:, at], rc_b.at[:, at], "gx_1", 1 - c, "core", ("b", d))

    def ready_a(d):
        arrived(("a", d))
        each_a((y + d) % 4, c, put_in(acc_a, rc_a))

    def ready_b(d):
        arrived(("b", d))
        each_b((x + d) % 4, c, put_in(acc_b, rc_b))

    def add(dst, *srcs):
        for j in range(dst.shape[0]):
            value = dst[j].astype(F32)
            for src in srcs:
                value = value + src[j].astype(F32)
            dst[j] = value.astype(BF)

    class Reduce:
        def __init__(self, name, axis1, p1, axis2, p2, acc, tr1, rx1, tr2, rx2, ready):
            self.name, self.axis1, self.p1, self.axis2, self.p2 = name, axis1, p1, axis2, p2
            self.acc, self.tr1, self.rx1, self.tr2, self.rx2, self.ready = acc, tr1, rx1, tr2, rx2, ready

        def sub(self, d1, d2):
            return self.acc.at[(self.p1 + d1) % 4, (self.p2 + d2) % 4]

        def first(self, turn, src, dst, *into):
            send(src, dst, self.axis1, (self.p1 + turn) % 4, "ring1", (self.name, *into))

        def second(self, turn, src, dst, *into):
            send(src, dst, self.axis2, (self.p2 + turn) % 4, "ring2", (self.name, *into))

        def s1(self, d):
            self.ready(d)
            k = order.index(d)
            self.first(1, self.sub(2, d).at[0:2], self.tr1.at[0, k], "u", d)
            self.first(3, self.sub(2, d).at[2:4], self.tr1.at[1, k], "d", d)
            self.first(1, self.sub(1, d).at[2:4], self.rx1.at[0, k, 2:4], "r", d)
            self.first(3, self.sub(3, d).at[0:2], self.rx1.at[1, k, 0:2], "r", d)

        def s2(self, d):
            k = order.index(d)
            arrived((self.name, "u", d))
            add(self.sub(1, d).at[0:2], self.tr1.at[0, k])
            self.first(1, self.sub(1, d).at[0:2], self.rx1.at[0, k, 0:2], "r", d)
            arrived((self.name, "d", d))
            add(self.sub(3, d).at[2:4], self.tr1.at[1, k])
            self.first(3, self.sub(3, d).at[2:4], self.rx1.at[1, k, 2:4], "r", d)

        def s3(self, d):
            k = order.index(d)
            arrived((self.name, "r", d))
            mine = self.sub(0, d)
            add(mine, self.rx1.at[0, k], self.rx1.at[1, k])
            if d == 2:
                self.second(1, mine.at[0:2], self.tr2.at[0], "u2")
                self.second(3, mine.at[2:4], self.tr2.at[1], "d2")
            if d == 1:
                self.second(1, mine.at[2:4], self.rx2.at[0, 2:4], "r2")
            if d == 3:
                self.second(3, mine.at[0:2], self.rx2.at[1, 0:2], "r2")

        def u3(self):
            arrived((self.name, "u2"))
            add(self.sub(0, 1).at[0:2], self.tr2.at[0])
            self.second(1, self.sub(0, 1).at[0:2], self.rx2.at[0, 0:2], "r2")
            arrived((self.name, "d2"))
            add(self.sub(0, 3).at[2:4], self.tr2.at[1])
            self.second(3, self.sub(0, 3).at[2:4], self.rx2.at[1, 2:4], "r2")

        def u4(self, at):
            arrived((self.name, "r2"))
            mine = self.sub(0, 0)
            for j in range(4):
                zb[at + j] = (mine[j].astype(F32) + self.rx2[0, j].astype(F32) + self.rx2[1, j].astype(F32)).astype(BF)

    both_rings = (
        Reduce("A", "gx_0", x, "gz", y, acc_a, tr_a, rx_a, tr_c, rx_c, ready_a),
        Reduce("B", "gz", y, "gx_0", x, acc_b, tr_b, rx_b, tr_d, rx_d, ready_b),
    )
    def each(method, d):
        for r in both_rings:
            getattr(r, method)(d)

    each("s1", 2)
    each("s1", 1)
    fill(early)
    next(gather_x)
    each("s2", 2)
    each("s1", 3)
    next(gather_x)
    each("s2", 1)
    each("s1", 0)
    fill(early)
    next(gather_x)
    each("s2", 3)
    next(gather_x)
    fill(early)
    each("s2", 0)
    each("s3", 2)
    next(gather_x)
    for d in (1, 3, 0):
        each("s3", d)
    for r in both_rings:
        r.u3()
    next(gather_x)
    fill(early)
    for i, r in enumerate(both_rings):
        r.u4(4 * i)

    for d in (4, 3, 5, 2, 6, 1, 7):
        send(zb.at[(z + d) % 8], zr.at[d - 1], "gy", (z + d) % 8, "z", "z")
    fill(early)
    next(gather_x)
    fill(early, 3)
    arrived("z")
    total = zb[z].astype(F32)
    for d in range(7):
        total = total + zr[d].astype(F32)
    domain = unpack(total).astype(BF)
    coupled = dot(domain, x_sq[...])
    gc[x, c, z // 4, y, z % 4] = pack(coupled).astype(BF)

    def across(ref):
        send(ref, ref, "gx_1", 1 - c, "over", "over")

    class Gather:
        def __init__(self, name, axis2, p2, axis3, p3, sub):
            self.name, self.axis2, self.p2, self.axis3, self.p3 = name, axis2, p2, axis3, p3
            self.at = sub

        def sub(self, d3, d2):
            return self.at((self.p3 + d3) % 4, (self.p2 + d2) % 4)

        def turn2(self, ref, d, *into):
            send(ref, ref, self.axis2, (self.p2 + d) % 4, "turn2", ("g" + self.name, *into))

        def turn3(self, ref, d, *into):
            send(ref, ref, self.axis3, (self.p3 + d) % 4, "turn3", ("g" + self.name, *into))

        def arrived(self, *into):
            arrived(("g" + self.name, *into))

        def spread(self, d):
            ref = self.sub(0, d)
            self.turn3(ref, 1, "u", d)
            self.turn3(ref, 3, "d", d)
            across(ref)

        def t0(self):
            ref = self.sub(0, 0)
            self.turn2(ref, 1, "u")
            self.turn2(ref, 3, "d")

        def t1(self):
            self.arrived("u")
            self.turn2(self.sub(0, 3).at[0:2], 1, "far")
            self.arrived("d")
            self.turn2(self.sub(0, 1).at[2:4], 3, "far")

        def t3(self):
            self.arrived("far")
            self.spread(2)

        def on(self, d):
            self.arrived("u", d)
            ref = self.sub(3, d)
            self.turn3(ref.at[0:2], 1, "far", d)
            across(ref)
            self.arrived("d", d)
            ref = self.sub(1, d)
            self.turn3(ref.at[2:4], 3, "far", d)
            across(ref)

        def last(self, d):
            self.arrived("far", d)
            across(self.sub(2, d))

    own = gc.at[x, c, z // 4, y, z % 4]
    for d in (4, 3, 5, 2, 6, 1, 7):
        send(own, own, "gy", (z + d) % 8, "z", "gz")
    fill(early, 12)
    next(gather_x)
    arrived("gz")
    both_rings = (
        Gather("A", "gz", y, "gx_0", x, lambda i3, i2: gc.at[i3, c, 0, i2]),
        Gather("B", "gx_0", x, "gz", y, lambda i3, i2: gc.at[i2, c, 1, i3]),
    )
    for r in both_rings:
        r.t0()
    for r in both_rings:
        r.spread(0)
    for r in both_rings:
        r.t1()
    for d in (3, 1):
        for r in both_rings:
            r.spread(d)
    for r in both_rings:
        r.on(0)
    for _ in gather_x:
        pass
    fill(late)
    for r in both_rings:
        r.t3()
    fill(late)
    for d in (3, 1):
        for r in both_rings:
            r.on(d)
    for r in both_rings:
        r.last(0)
    fill(late)
    for r in both_rings:
        r.on(2)
    fill(late)
    for d in (3, 1, 2):
        for r in both_rings:
            r.last(d)
    arrived("over")

    for g in range(groups):
        @pl.loop(0, 8 // UNROLL)
        def _(i):
            def right(u):
                at = 8 * g + UNROLL * i + u
                combined = (both(of_coupled, at) - pq[at].astype(F32)).astype(BF)
                w_sq[u, 0:R, :] = dot(combined, s_sq[at]).astype(BF)

            def left(u):
                at = 8 * g + UNROLL * i + u
                result = jnp.where(far < (ranks[at] + 1) * RSTEP, base[at] + dot(m_sq[at, 0:R, :], w_sq[u]), 0.0)
                tmp[u, 0] = result[:, 0:128]
                tmp[u, 1] = result[:, 128:256]

            def flat(u):
                p = UNROLL * i + u
                low = low_lanes(96)
                el, er, ol, oh = (tmp[u, j, pl.ds(e, 96, stride=2), :] for e in range(2) for j in range(2))
                ol, oh = pltpu.roll(ol, 64, 1), pltpu.roll(oh, 64, 1)
                lines[pl.ds(p, 96, stride=24), :] = el
                lines[pl.ds(8 + p, 96, stride=24), :] = jnp.where(low, er, ol)
                lines[pl.ds(16 + p, 96, stride=24), :] = jnp.where(low, ol, oh)

            skewed(UNROLL, right, left, flat)

        @pl.loop(0, LINES // 36)
        def _(i):
            for u in range(36):
                at = i * 36 + u
                o_ref[8 * g : 8 * g + 8, pl.ds(pl.multiple_of(at * 128, 128), 128)] = lines[
                    pl.ds(pl.multiple_of(at * 8, 8), 8), :
                ].astype(BF)

    assert len(leaving) == OUT and len(arriving) == INTO
    for index, size in leaving.values():
        await_all(send_sem.at[index], size)


def store_kernel(r_ref, o_hbm, sem):
    copies = []
    for g in range(r_ref.shape[0] // 8):
        copy = pltpu.make_async_copy(r_ref.at[8 * g : 8 * g + 8], o_hbm.at[8 * g : 8 * g + 8], sem.at[g])
        copy.start()
        copies.append(copy)
    for copy in copies:
        copy.wait()


def body(pair_list, rank_bucket, amplitudes, intersects, integrals, exchange_blocks):
    n = amplitudes.shape[0]
    hbm = pl.BlockSpec(memory_space=pl.ANY)

    def held(array):
        return pltpu.with_memory_space_constraint(array, pltpu.HBM)

    vmem = pl.BlockSpec(memory_space=pltpu.VMEM)
    tail = (CH, 128)
    residuals = pl.pallas_call(
        kernel,
        in_specs=[hbm] * 6,
        out_specs=vmem,
        out_shape=jax.ShapeDtypeStruct((n, R * R), BF),
        scratch_shapes=[
            *[pltpu.VMEM((n, R * R), BF)] * 2,
            pltpu.VMEM((1, R * R), BF),
            *[pltpu.VMEM((LINES * 8, 128), F32)] * 2,
            pltpu.VMEM((LINES, 128), F32),
            pltpu.VMEM((UNROLL, 2, R, 128), F32),
            pltpu.VMEM((n, W, W), BF),
            pltpu.VMEM((n, W, W), BF),
            pltpu.VMEM((2, W, W), BF),
            pltpu.VMEM((W, W), BF),
            pltpu.VMEM((UNROLL, W, W), BF),
            pltpu.VMEM((n, R, W), BF),
            pltpu.VMEM((n, R, W), F32),
            pltpu.VMEM((n + 1, 4) + tail, BF),
            pltpu.VMEM((4, 2, 2, 4, 4) + tail, BF),
            pltpu.VMEM((4, 2, 8, 4) + tail, BF),
            *[pltpu.VMEM((4, 4, 4) + tail, BF)] * 6,
            *[pltpu.VMEM((2, 4, 2) + tail, BF), pltpu.VMEM((2, 4, 4) + tail, BF)] * 2,
            *[pltpu.VMEM((2, 2) + tail, BF), pltpu.VMEM((2, 4) + tail, BF)] * 2,
            pltpu.VMEM((8,) + tail, BF),
            pltpu.VMEM((7,) + tail, BF),
            pltpu.VMEM((2, 128), jnp.int32),
            pltpu.SMEM((2, 128), jnp.int32),
            pltpu.SMEM((2, n), jnp.int32),
            pltpu.SMEM((n,), jnp.int32),
            pltpu.SemaphoreType.DMA((3, n // 8)),
            pltpu.SemaphoreType.DMA((4,)),
            pltpu.SemaphoreType.DMA((OUT,)),
            pltpu.SemaphoreType.DMA((INTO,)),
        ],
        compiler_params=pltpu.CompilerParams(collective_id=0, has_side_effects=True, vmem_limit_bytes=50 * 2**20),
    )(held(pair_list.T), held(rank_bucket), amplitudes, intersects, integrals, held(exchange_blocks))
    return pl.pallas_call(
        store_kernel,
        in_specs=[vmem],
        out_specs=hbm,
        out_shape=jax.ShapeDtypeStruct((n, R * R), BF),
        scratch_shapes=[pltpu.SemaphoreType.DMA((n // 8,))],
        compiler_params=pltpu.CompilerParams(vmem_limit_bytes=4 * 2**20),
    )(residuals)


def solution(mesh):
    torus = Mesh(mesh.devices.reshape(4, 2, mesh.shape["gy"], mesh.shape["gz"]), GX_GY_GZ)
    return jax.shard_map(
        body,
        mesh=torus,
        in_specs=(
            P(GX_GY_GZ, None),
            P(GX_GY_GZ),
            P(GX_GY_GZ, None),
            P(GX_GY_GZ, None),
            P(GX_GY_GZ, None),
            P(GX_GY, None),
        ),
        out_specs=P(GX_GY_GZ, None),
        check_vma=False,
    )
```
